32 devices in a mesh: grp: 2 (over y), lat: 4 (over z), lay: 4 (over x, core).
Axes of the slice: x: 2, y: 2, z: 4, core: 2. Of those that a mesh axis runs over, the one named last changes fastest.
Arguments:
- acts: bfloat16 [128, 4, 1280], P(('grp', 'lat'), 'lay'), parts along dimension 0, may hold values from -6 to 6
- w_enc: bfloat16 [4, 1280, 1536], P('lay', None, 'lat'), may hold values from -0.078125 to 0.078125
- w_dec: bfloat16 [1536, 4, 1280], P('lat', 'lay'), may hold values from -0.15625 to 0.15625
- b_enc: float32 [1536], P('lat'), may hold values from -3 to 3
- b_dec: float32 [4, 1280], P('lay'), may hold values from -3 to 3
Outputs:
- lat_grad: bfloat16 [128, 1536], P('grp', 'lat'), parts along dimension 0
- enc_grad: bfloat16 [8, 1280, 1536], P(('grp', 'lay'), None, 'lat'), parts along dimension 0
- dec_grad: bfloat16 [1536, 8, 1280], P('lat', ('grp', 'lay')), parts along dimension 1
The draws below stay inside these ranges and needn't reach their ends.
There are 2 independent parts, one for each index of `grp`. The reference program is written for one: setup_inputs(seed, part) draws one part's arguments, and reference() takes and returns one part's arrays. A program takes and returns all parts, laid end to end along the dimension named above; an argument that names none is the same for every part. Nothing has to cross between parts.
All inputs are finite; a program needn't handle non-finite values.
Results may differ from the reference program's by a relative error of at most 0.023.
Values may be sent and summed in bfloat16 or wider, within the bound.
A program may use at most 64 MiB of HBM per device.

```python
import jax
import jax.numpy as jnp

D = 1280
LATENTS = 1536
LAYERS = 4
ROWS = 64


def levels(stream_key, extent, pieces, least, top_value):
    def one(dim, parts):
        heights = jax.random.uniform(jax.random.fold_in(jax.random.fold_in(stream_key, 6), dim), (parts,), jnp.float32, least / len(pieces), top_value / len(pieces))
        return jnp.repeat(jnp.exp(heights), extent[dim] // parts).reshape((-1,) + (1,) * (len(extent) - dim - 1))

    level = one(*pieces[0])
    for cut in pieces[1:]:
        level = level * one(*cut)
    return level


def noise(key, dims, width, most, shards=(), held_as=jnp.bfloat16):
    array = width * jax.random.normal(key, dims, jnp.float32)
    if shards:
        array = array * levels(key, dims, shards, -0.22, 0.18)
    return jnp.clip(array, -most, most).astype(held_as)


def setup_inputs(seed: int = 0, part: int = 0) -> dict:
    streams_of = jax.random.split(jax.random.key(seed), 6)
    part_splits = jax.random.split(jax.random.fold_in(streams_of[5], part), 6)
    return {
        "acts": noise(part_splits[0], (ROWS, LAYERS, D), 1.0, 6.0, ((0, 4), (1, 4))),
        "w_enc": noise(streams_of[1], (LAYERS, D, LATENTS), (LAYERS * D) ** -0.5, 0.078125, ((0, 4), (2, 4))),
        "w_dec": noise(streams_of[2], (LATENTS, LAYERS, D), LATENTS ** -0.5, 0.15625, ((0, 4), (1, 4))),
        "b_enc": noise(streams_of[3], (LATENTS,), 0.5, 3.0, ((0, 4),), jnp.float32),
        "b_dec": noise(streams_of[4], (LAYERS, D), 0.5, 3.0, ((0, 4),), jnp.float32),
    }


def reference(acts, w_enc, w_dec, b_enc, b_dec):
    x32 = acts.astype(jnp.float32)
    pre = jnp.einsum("bld,ldm->bm", x32, w_enc.astype(jnp.float32)) + b_enc[None, :]
    code = (jax.nn.softplus(4.0 * pre) / 4.0).astype(jnp.bfloat16)
    slope = jax.nn.sigmoid(4.0 * pre)
    recon = jnp.einsum("bm,mld->bld", code.astype(jnp.float32), w_dec.astype(jnp.float32))
    err = (recon + b_dec[None, :, :] - x32).astype(jnp.bfloat16)
    back = jnp.einsum("bld,mld->bm", err.astype(jnp.float32), w_dec.astype(jnp.float32))
    lat_grad = (back * slope).astype(jnp.bfloat16)
    enc_grad = jnp.einsum("bld,bm->ldm", x32, lat_grad.astype(jnp.float32)).astype(jnp.bfloat16)
    dec_grad = jnp.einsum("bm,bld->mld", code.astype(jnp.float32), err.astype(jnp.float32)).astype(jnp.bfloat16)
    return lat_grad, enc_grad, dec_grad
```

```python
import functools

import jax
import jax.numpy as jnp
from jax import lax
from jax.experimental import pallas as pl
from jax.experimental.pallas import tpu as pltpu
from jax.sharding import PartitionSpec as P

MESH = pl.DeviceIdType.MESH
F32, BF16 = jnp.float32, jnp.bfloat16


def flip(v, j):
    out, bit = v, 1
    while bit <= j:
        if j & bit:
            out = out + bit * (1 - 2 * lax.rem(lax.div(v, bit), 2))
        bit *= 2
    return out


def step(
    n_lat, n_lay, groups, acts_hbm, wenc_hbm, wdec_hbm, benc_ref, bdec_ref,
    lat_out, acts_t, dec_out,
    acts_all, wenc, wdec, wdec_t, pre_buf, back_buf, rec_mine, rec_buf, err_all, code_all, slope,
    load, acts_s, acts_r, pre_s, pre_r, rec_s, rec_r, err_s, err_r, back_s, back_r,
):
    z, l = lax.axis_index("lat"), lax.axis_index("lay")
    row_dev, wide = acts_all.shape[1:]
    rows, lat_dev = n_lat * row_dev, wenc.shape[1]
    size = n_lat // groups
    part = size * row_dev

    load_acts = pltpu.make_async_copy(acts_hbm, acts_all.at[z], load.at[0])
    load_enc = pltpu.make_async_copy(wenc_hbm, wenc, load.at[1])
    load_dec = pltpu.make_async_copy(wdec_hbm, wdec, load.at[2])
    load_acts.start()
    load_enc.start()
    load_dec.start()

    if groups > 1:
        dest = source = lambda j: flip(z, j)
    else:
        dest = lambda j: lax.rem(z + j, n_lat)
        source = lambda j: lax.rem(z + n_lat - j, n_lat)
    group = [flip(lax.div(z, size), g) if groups > 1 else 0 for g in range(groups)]

    def lay_peer(k):
        return {"lay": lax.rem(l + k, n_lay)}

    barrier = pltpu.get_barrier_semaphore()
    for j in reversed(range(1, n_lat)):
        pl.semaphore_signal(
            barrier, inc=1, device_id={"lat": dest(j)}, device_id_type=MESH
        )
    for k in range(1, n_lay):
        pl.semaphore_signal(barrier, inc=1, device_id=lay_peer(k), device_id_type=MESH)
    pl.semaphore_wait(barrier, n_lat + n_lay - 2)

    started = []

    def send(src, dst, send_sem, recv_sem, peer):
        copy = pltpu.make_async_remote_copy(
            src_ref=src, dst_ref=dst, send_sem=send_sem, recv_sem=recv_sem,
            device_id=peer, device_id_type=MESH,
        )
        copy.start()
        started.append(copy)
        return copy

    def to_lat(buf, sent, received):
        return {
            j: send(buf.at[z], buf.at[z], sent.at[j], received.at[j], {"lat": dest(j)})
            for j in range(1, n_lat)
        }

    def to_lay(buf, g, sent, received):
        block = buf.at[l, group[g]]
        return [
            send(block, block, sent.at[g, k], received.at[g, k], lay_peer(k))
            for k in range(1, n_lay)
        ]

    def arrive(copies, g):
        for j in range(g * size, (g + 1) * size):
            if j:
                copies[j].wait_recv()

    def rows_of(buf, g):
        return buf[pl.ds(group[g] * size, size)].reshape(part, wide)

    def total(buf, g):
        whole = buf[0, group[g]].astype(F32)
        for i in range(1, n_lay):
            whole += buf[i, group[g]].astype(F32)
        return whole

    load_acts.wait()
    acts_copies = to_lat(acts_all, acts_s, acts_r)
    load_enc.wait()
    pre_copies, rec_copies = {}, {}

    def encode(g):
        arrive(acts_copies, g)
        pre = jnp.dot(rows_of(acts_all, g), wenc[...], preferred_element_type=F32)
        pre_buf[l, group[g]] = pre.astype(BF16)
        pre_copies[g] = to_lay(pre_buf, g, pre_s, pre_r)

    def decode(g):
        for copy in pre_copies[g]:
            copy.wait_recv()
        x = 4.0 * (total(pre_buf, g) + benc_ref[...].reshape(1, lat_dev))
        e = jnp.exp(-jnp.abs(x))
        code = (0.25 * (jnp.maximum(x, 0.0) + jnp.log1p(e))).astype(BF16)
        rec = jnp.dot(code, wdec[...], preferred_element_type=F32).astype(BF16)
        rec_mine[pl.ds(group[g] * size, size)] = rec.reshape(size, row_dev, wide)
        for j in range(g * size, (g + 1) * size):
            if j:
                rec_copies[j] = send(
                    rec_mine.at[dest(j)], rec_buf.at[z], rec_s.at[j], rec_r.at[j],
                    {"lat": dest(j)},
                )
        code_all[group[g]] = code
        slope[group[g]] = jnp.where(x >= 0.0, 1.0, e) / (1.0 + e)

    for g in range(groups):
        encode(g)
        if g == 0:
            load_dec.wait()
    for g in [*range(1, groups), 0]:
        decode(g)
    wdec_t[...] = wdec[...].astype(F32).T.astype(BF16)
    acts_t[...] = acts_all[...].reshape(rows, wide).astype(F32).T.astype(BF16)
    code_t = code_all[...].reshape(rows, lat_dev).astype(F32).T.astype(BF16)
    err = bdec_ref[...] - acts_all[z].astype(F32) + rec_mine[z].astype(F32)
    for j in range(1, n_lat):
        rec_copies[j].wait_recv()
        err += rec_buf[source(j)].astype(F32)
    err_all[z] = err.astype(BF16)
    err_copies = to_lat(err_all, err_s, err_r)
    back_copies = {}
    for g in range(groups):
        arrive(err_copies, g)
        back = jnp.dot(rows_of(err_all, g), wdec_t[...], preferred_element_type=F32)
        back_buf[l, group[g]] = back.astype(BF16)
        back_copies[g] = to_lay(back_buf, g, back_s, back_r)
    errs = err_all[...].reshape(rows, wide)
    dec_out[...] = jnp.dot(code_t, errs, preferred_element_type=F32).astype(BF16)
    for g in range(groups):
        for copy in back_copies[g]:
            copy.wait_recv()
        lat_out[group[g]] = (total(back_buf, g) * slope[group[g]]).astype(BF16)
    for copy in started:
        copy.wait_send()


def same(v, c):
    return lax.div(1, 1 + (v - c) * (v - c))


def line_step(
    n_lat, n_lay, acts_hbm, wenc_hbm, wdec_hbm, benc_hbm, bdec_hbm,
    lat_out, acts_t, dec_out,
    acts_all, wenc, wdec, wdec_t, benc, bdec, pre_buf, back_buf, rec_mine, rec_buf, err_all,
    code_all, slope,
    load, acts_s, acts_r, pre_s, pre_r, rec_s, rec_r, err_s, err_r, back_s, back_r,
):
    z, l = lax.axis_index("lat"), lax.axis_index("lay")
    row_dev, wide = acts_all.shape[1:]
    rows, lat_dev = n_lat * row_dev, wenc.shape[1]
    half = n_lat // 2
    high, low = half, half - 1
    upper = lax.div(z, half)
    place = z + upper * (n_lat - 1 - 2 * z)

    def farthest(k):
        v = n_lat - 1 - k
        v = v - (1 - lax.div(1, 1 + lax.div(place, v)))
        return v + upper * (n_lat - 1 - 2 * v)

    def lay_peer(k):
        return {"lay": flip(l, k)}

    barrier = pltpu.get_barrier_semaphore()
    for k in range(n_lat - 1):
        pl.semaphore_signal(
            barrier, inc=1, device_id={"lat": farthest(k)}, device_id_type=MESH
        )
    for k in reversed(range(1, n_lay)):
        pl.semaphore_signal(barrier, inc=1, device_id=lay_peer(k), device_id_type=MESH)

    load_acts = pltpu.make_async_copy(acts_hbm, acts_all.at[z], load.at[0])
    load_enc = pltpu.make_async_copy(wenc_hbm, wenc, load.at[1])
    load_dec = pltpu.make_async_copy(wdec_hbm, wdec, load.at[2])
    load_benc = pltpu.make_async_copy(benc_hbm, benc, load.at[3])
    load_bdec = pltpu.make_async_copy(bdec_hbm, bdec, load.at[4])
    load_acts.start()
    load_enc.start()
    load_dec.start()
    load_benc.start()
    load_bdec.start()

    pl.semaphore_wait(barrier, n_lat + n_lay - 2)

    def send(src, dst, send_sem, recv_sem, peer):
        pltpu.make_async_remote_copy(
            src_ref=src, dst_ref=dst, send_sem=send_sem, recv_sem=recv_sem,
            device_id=peer, device_id_type=MESH,
        ).start()

    def wait(view, sem):
        pltpu.make_async_copy(view, view, sem).wait()

    def to_lay(buf, k, sent, received):
        for j in sorted(range(1, n_lay), key=lambda j: (j < 2, j)):
            send(buf.at[k, 0], buf.at[k, j], sent, received.at[k], lay_peer(j))

    def total(buf, k, received):
        wait(buf.at[k, pl.ds(1, n_lay - 1)], received.at[k])
        whole = buf[k, l].astype(F32)
        for i in range(1, n_lay):
            whole += buf[k, flip(l, i)].astype(F32)
        return whole

    first = [
        z + k - (1 - lax.div(1, 1 + lax.div(z + k, n_lat))) * (z + 2 * k + 1 - n_lat)
        for k in range(n_lat)
    ]

    load_acts.wait()
    for k in range(n_lat - 1):
        send(acts_all.at[z], acts_all.at[z], acts_s, acts_r.at[z], {"lat": farthest(k)})
    load_enc.wait()

    def encode(k):
        if k:
            wait(acts_all.at[first[k]], acts_r.at[first[k]])
        pre = jnp.dot(acts_all[first[k]], wenc[...], preferred_element_type=F32)
        pre_buf[k, 0] = pre.astype(BF16)
        to_lay(pre_buf, k, pre_s, pre_r)

    def decode(k):
        b = first[k]
        x = 4.0 * (total(pre_buf, k, pre_r) + benc[...].reshape(1, lat_dev))
        e = jnp.exp(-jnp.abs(x))
        code = (0.25 * (jnp.maximum(x, 0.0) + jnp.log1p(e))).astype(BF16)
        rec = jnp.dot(code, wdec[...], preferred_element_type=F32).astype(BF16)
        rec_mine[b] = rec
        owner = high - lax.div(b, half)

        @pl.when(owner != z)
        def _():
            place = lax.rem(b, half)
            send(rec_mine.at[b], rec_buf.at[place, z], rec_s, rec_r.at[place], {"lat": owner})

        code_all[b] = code
        slope[b] = jnp.where(x >= 0.0, 1.0, e) / (1.0 + e)

    encode(0)
    load_dec.wait()
    wdec_t[...] = wdec[...].astype(F32).T.astype(BF16)
    for k in range(1, n_lat):
        encode(k)
    acts_t[...] = acts_all[...].reshape(rows, wide).astype(F32).T.astype(BF16)
    load_benc.wait()
    load_bdec.wait()
    for k in range(n_lat):
        decode(k)

    @pl.when((z == low) | (z == high))
    def _():
        for j in range(half):
            b = half + j - same(z, high) * (2 * j + 1)
            place = lax.rem(b, half)
            wait(rec_buf.at[place, pl.ds(0, n_lat - 1)], rec_r.at[place])
            err = bdec[...] - acts_all[b].astype(F32) + rec_mine[b].astype(F32)
            for i in range(1, n_lat):
                err += rec_buf[place, flip(z, i)].astype(F32)
            err_all[b] = err.astype(BF16)
            for k in range(n_lat - 1):
                send(err_all.at[b], err_all.at[b], err_s, err_r.at[b], {"lat": farthest(k)})

    code_t = code_all[...].reshape(rows, lat_dev).astype(F32).T.astype(BF16)
    second = []
    for k in range(n_lat):
        up = half + k if k < half else n_lat - 1 - k
        down = half - 1 - k if k < half else k
        b = up + same(z, high) * (down - up)
        second.append(b)
        owner = high - lax.div(b, half)

        @pl.when(owner != z)
        def _():
            wait(err_all.at[b], err_r.at[b])

        back = jnp.dot(err_all[b], wdec_t[...], preferred_element_type=F32)
        back_buf[k, 0] = back.astype(BF16)
        to_lay(back_buf, k, back_s, back_r)
    errs = err_all[...].reshape(rows, wide)
    dec_out[...] = jnp.dot(code_t, errs, preferred_element_type=F32).astype(BF16)
    for k in range(n_lat):
        b = second[k]
        lat_out[b] = (total(back_buf, k, back_r) * slope[b]).astype(BF16)

    wait(acts_all.at[pl.ds(0, n_lat - 1)], acts_s)
    wait(pre_buf.at[:, pl.ds(1, n_lay - 1)], pre_s)
    wait(back_buf.at[:, pl.ds(1, n_lay - 1)], back_s)

    @pl.when((z == low) | (z == high))
    def _():
        wait(rec_mine.at[pl.ds(0, half)], rec_s)
        wait(rec_buf.at[:, pl.ds(0, n_lat - 1)], err_s)

    @pl.when((z != low) & (z != high))
    def _():
        wait(rec_mine, rec_s)


def finish(chunks, lat, acts_t, dec, lat_hbm, enc_hbm, dec_hbm, enc, sems):
    rows, lat_dev = lat.shape[0] * lat.shape[1], lat.shape[2]
    copies = [
        pltpu.make_async_copy(dec, dec_hbm, sems.at[0]),
        pltpu.make_async_copy(lat, lat_hbm, sems.at[1]),
    ]
    for copy in copies:
        copy.start()
    grad = lat[...].reshape(rows, lat_dev)
    tall = enc.shape[0] // chunks
    for c in range(chunks):
        cut = pl.ds(c * tall, tall)
        enc[cut] = jnp.dot(acts_t[cut], grad, preferred_element_type=F32).astype(BF16)
        copy = pltpu.make_async_copy(enc.at[cut], enc_hbm.at[cut], sems.at[2 + c])
        copy.start()
        copies.append(copy)
    for copy in copies:
        copy.wait()


def solution(mesh):
    n_lat, n_lay = mesh.shape["lat"], mesh.shape["lay"]

    def on_device(acts, w_enc, w_dec, b_enc, b_dec):
        row_dev, lay_dev, width = acts.shape
        lat_dev = w_enc.shape[2]
        wide, rows = lay_dev * width, n_lat * row_dev
        hbm = pl.BlockSpec(memory_space=pltpu.HBM)
        vmem = pl.BlockSpec(memory_space=pltpu.VMEM)
        dma = pltpu.SemaphoreType.DMA
        line = n_lat in (2, 4) and n_lay & (n_lay - 1) == 0
        groups = 4 if n_lat & (n_lat - 1) == 0 and n_lat % 4 == 0 else 1
        if line:
            groups = n_lat
        part = rows // groups
        chunks = 5 if wide % 80 == 0 else 1
        out_shape = [
            pltpu.VMEM((groups, part, lat_dev), BF16),
            pltpu.VMEM((wide, rows), BF16),
            pltpu.VMEM((lat_dev, wide), BF16),
        ]
        rows_buf = pltpu.VMEM((n_lat, row_dev, wide), BF16)
        if line:
            kernel = functools.partial(line_step, n_lat, n_lay)
            in_specs = [hbm] * 5
            lay_buf = pltpu.VMEM((groups, n_lay, part, lat_dev), BF16)
            scratch = [
                rows_buf,
                pltpu.VMEM((wide, lat_dev), BF16),
                pltpu.VMEM((lat_dev, wide), BF16),
                pltpu.VMEM((wide, lat_dev), BF16),
                pltpu.VMEM((lat_dev,), F32),
                pltpu.VMEM((1, wide), F32),
                lay_buf,
                lay_buf,
                rows_buf,
                pltpu.VMEM((n_lat // 2, n_lat, row_dev, wide), BF16),
                rows_buf,
                pltpu.VMEM((groups, part, lat_dev), BF16),
                pltpu.VMEM((groups, part, lat_dev), F32),
                dma((5,)),
                dma, dma((n_lat,)),
                dma, dma((groups,)),
                dma, dma((n_lat // 2,)),
                dma, dma((n_lat,)),
                dma, dma((groups,)),
            ]
        else:
            kernel = functools.partial(step, n_lat, n_lay, groups)
            in_specs = [hbm, hbm, hbm, vmem, vmem]
            scratch = [
                rows_buf,
                pltpu.VMEM((wide, lat_dev), BF16),
                pltpu.VMEM((lat_dev, wide), BF16),
                pltpu.VMEM((wide, lat_dev), BF16),
                pltpu.VMEM((n_lay, groups, part, lat_dev), BF16),
                pltpu.VMEM((n_lay, groups, part, lat_dev), BF16),
                rows_buf,
                rows_buf,
                rows_buf,
                pltpu.VMEM((groups, part, lat_dev), BF16),
                pltpu.VMEM((groups, part, lat_dev), F32),
                dma((3,)),
                dma((n_lat,)), dma((n_lat,)),
                dma((groups, n_lay)), dma((groups, n_lay)),
                dma((n_lat,)), dma((n_lat,)),
                dma((n_lat,)), dma((n_lat,)),
                dma((groups, n_lay)), dma((groups, n_lay)),
            ]
        lat_part, acts_t, dec_part = pl.pallas_call(
            kernel,
            out_shape=out_shape,
            in_specs=in_specs,
            out_specs=[vmem, vmem, vmem],
            scratch_shapes=scratch,
            compiler_params=pltpu.CompilerParams(collective_id=0, has_side_effects=True),
            cost_estimate=pl.CostEstimate(
                flops=8 * rows * wide * lat_dev,
                bytes_accessed=4 * wide * lat_dev,
                transcendentals=0,
            ),
        )(
            acts.reshape(row_dev, wide),
            w_enc.reshape(wide, lat_dev),
            w_dec.reshape(lat_dev, wide),
            b_enc,
            b_dec.reshape(1, wide),
        )
        lat_grad, enc_grad, dec_grad = pl.pallas_call(
            functools.partial(finish, chunks),
            out_shape=[
                jax.ShapeDtypeStruct((groups, part, lat_dev), BF16),
                jax.ShapeDtypeStruct((wide, lat_dev), BF16),
                jax.ShapeDtypeStruct((lat_dev, wide), BF16),
            ],
            in_specs=[vmem, vmem, vmem],
            out_specs=[hbm, hbm, hbm],
            scratch_shapes=[pltpu.VMEM((wide, lat_dev), BF16), dma((2 + chunks,))],
            compiler_params=pltpu.CompilerParams(vmem_limit_bytes=8 * wide * lat_dev),
            cost_estimate=pl.CostEstimate(
                flops=2 * rows * wide * lat_dev,
                bytes_accessed=4 * wide * lat_dev,
                transcendentals=0,
            ),
        )(lat_part, acts_t, dec_part)
        return (
            lat_grad.reshape(rows, lat_dev),
            enc_grad.reshape(lay_dev, width, lat_dev),
            dec_grad.reshape(lat_dev, lay_dev, width),
        )

    in_specs = (
        P(("grp", "lat"), "lay", None),
        P("lay", None, "lat"),
        P("lat", "lay", None),
        P("lat"),
        P("lay", None),
    )
    out_specs = (P("grp", "lat"), P(("grp", "lay"), None, "lat"), P("lat", ("grp", "lay"), None))
    return jax.shard_map(
        on_device, mesh=mesh, in_specs=in_specs, out_specs=out_specs, check_vma=False
    )
```

```python
import functools

import jax
import jax.numpy as jnp
from jax import lax
from jax.experimental import pallas as pl
from jax.experimental.pallas import tpu as pltpu
from jax.sharding import PartitionSpec as P

MESH = pl.DeviceIdType.MESH
F32, BF16 = jnp.float32, jnp.bfloat16


def flip(v, j):
    out, bit = v, 1
    while bit <= j:
        if j & bit:
            out = out + bit * (1 - 2 * lax.rem(lax.div(v, bit), 2))
        bit *= 2
    return out


def step(
    n_lat, n_lay, groups, acts_hbm, wenc_hbm, wdec_hbm, benc_ref, bdec_ref,
    lat_out, acts_t, dec_out,
    acts_all, wenc, wdec, wdec_t, pre_buf, back_buf, rec_mine, rec_buf, err_all, code_all, slope,
    load, acts_s, acts_r, pre_s, pre_r, rec_s, rec_r, err_s, err_r, back_s, back_r,
):
    z, l = lax.axis_index("lat"), lax.axis_index("lay")
    row_dev, wide = acts_all.shape[1:]
    rows, lat_dev = n_lat * row_dev, wenc.shape[1]
    size = n_lat // groups
    part = size * row_dev

    load_acts = pltpu.make_async_copy(acts_hbm, acts_all.at[z], load.at[0])
    load_enc = pltpu.make_async_copy(wenc_hbm, wenc, load.at[1])
    load_dec = pltpu.make_async_copy(wdec_hbm, wdec, load.at[2])
    load_acts.start()
    load_enc.start()
    load_dec.start()

    if groups > 1:
        dest = source = lambda j: flip(z, j)
    else:
        dest = lambda j: lax.rem(z + j, n_lat)
        source = lambda j: lax.rem(z + n_lat - j, n_lat)
    group = [flip(lax.div(z, size), g) if groups > 1 else 0 for g in range(groups)]

    def lay_peer(k):
        return {"lay": lax.rem(l + k, n_lay)}

    barrier = pltpu.get_barrier_semaphore()
    for j in reversed(range(1, n_lat)):
        pl.semaphore_signal(
            barrier, inc=1, device_id={"lat": dest(j)}, device_id_type=MESH
        )
    for k in range(1, n_lay):
        pl.semaphore_signal(barrier, inc=1, device_id=lay_peer(k), device_id_type=MESH)
    pl.semaphore_wait(barrier, n_lat + n_lay - 2)

    started = []

    def send(src, dst, send_sem, recv_sem, peer):
        copy = pltpu.make_async_remote_copy(
            src_ref=src, dst_ref=dst, send_sem=send_sem, recv_sem=recv_sem,
            device_id=peer, device_id_type=MESH,
        )
        copy.start()
        started.append(copy)
        return copy

    def to_lat(buf, sent, received):
        return {
            j: send(buf.at[z], buf.at[z], sent.at[j], received.at[j], {"lat": dest(j)})
            for j in range(1, n_lat)
        }

    def to_lay(buf, g, sent, received):
        block = buf.at[l, group[g]]
        return [
            send(block, block, sent.at[g, k], received.at[g, k], lay_peer(k))
            for k in range(1, n_lay)
        ]

    def arrive(copies, g):
        for j in range(g * size, (g + 1) * size):
            if j:
                copies[j].wait_recv()

    def rows_of(buf, g):
        return buf[pl.ds(group[g] * size, size)].reshape(part, wide)

    def total(buf, g):
        whole = buf[0, group[g]].astype(F32)
        for i in range(1, n_lay):
            whole += buf[i, group[g]].astype(F32)
        return whole

    load_acts.wait()
    acts_copies = to_lat(acts_all, acts_s, acts_r)
    load_enc.wait()
    pre_copies, rec_copies = {}, {}

    def encode(g):
        arrive(acts_copies, g)
        pre = jnp.dot(rows_of(acts_all, g), wenc[...], preferred_element_type=F32)
        pre_buf[l, group[g]] = pre.astype(BF16)
        pre_copies[g] = to_lay(pre_buf, g, pre_s, pre_r)

    def decode(g):
        for copy in pre_copies[g]:
            copy.wait_recv()
        x = 4.0 * (total(pre_buf, g) + benc_ref[...].reshape(1, lat_dev))
        e = jnp.exp(-jnp.abs(x))
        code = (0.25 * (jnp.maximum(x, 0.0) + jnp.log1p(e))).astype(BF16)
        rec = jnp.dot(code, wdec[...], preferred_element_type=F32).astype(BF16)
        rec_mine[pl.ds(group[g] * size, size)] = rec.reshape(size, row_dev, wide)
        for j in range(g * size, (g + 1) * size):
            if j:
                rec_copies[j] = send(
                    rec_mine.at[dest(j)], rec_buf.at[z], rec_s.at[j], rec_r.at[j],
                    {"lat": dest(j)},
                )
        code_all[group[g]] = code
        slope[group[g]] = jnp.where(x >= 0.0, 1.0, e) / (1.0 + e)

    for g in range(groups):
        encode(g)
        if g == 0:
            load_dec.wait()
    for g in [*range(1, groups), 0]:
        decode(g)
    wdec_t[...] = wdec[...].astype(F32).T.astype(BF16)
    acts_t[...] = acts_all[...].reshape(rows, wide).astype(F32).T.astype(BF16)
    code_t = code_all[...].reshape(rows, lat_dev).astype(F32).T.astype(BF16)
    err = bdec_ref[...] - acts_all[z].astype(F32) + rec_mine[z].astype(F32)
    for j in range(1, n_lat):
        rec_copies[j].wait_recv()
        err += rec_buf[source(j)].astype(F32)
    err_all[z] = err.astype(BF16)
    err_copies = to_lat(err_all, err_s, err_r)
    back_copies = {}
    for g in range(groups):
        arrive(err_copies, g)
        back = jnp.dot(rows_of(err_all, g), wdec_t[...], preferred_element_type=F32)
        back_buf[l, group[g]] = back.astype(BF16)
        back_copies[g] = to_lay(back_buf, g, back_s, back_r)
    errs = err_all[...].reshape(rows, wide)
    dec_out[...] = jnp.dot(code_t, errs, preferred_element_type=F32).astype(BF16)
    for g in range(groups):
        for copy in back_copies[g]:
            copy.wait_recv()
        lat_out[group[g]] = (total(back_buf, g) * slope[group[g]]).astype(BF16)
    for copy in started:
        copy.wait_send()


def same(v, c):
    return lax.div(1, 1 + (v - c) * (v - c))


OWNER = [2, 2, 1, 0]
FIRST = [[0, 1, 2, 3], [1, 2, 3, 0], [2, 3, 1, 0], [3, 2, 1, 0]]
SECOND = [[3, 2, 1, 0], [2, 3, 1, 0], [0, 1, 2, 3], [1, 0, 2, 3]]
OWNED = [[3], [2], [1, 0], []]
TARGETS = [[3, 2, 1], [3, 2, 0], [0, 1, 3], [0, 1, 2]]
SPREAD = [[1, 2, 3], [3, 2, 0], [0, 1, 3], []]


def line_step(
    n_lat, n_lay, acts_hbm, wenc_hbm, wdec_hbm, benc_hbm, bdec_hbm,
    lat_out, acts_t, dec_out,
    acts_all, wenc, wdec, wdec_t, benc, bdec, pre_buf, back_buf, rec_mine, rec_buf, err_all,
    code_all, slope,
    load, acts_s, acts_r, pre_s, pre_r, rec_s, rec_r, err_s, err_r, back_s, back_r,
):
    z, l = lax.axis_index("lat"), lax.axis_index("lay")
    row_dev, wide = acts_all.shape[1:]
    rows, lat_dev = n_lat * row_dev, wenc.shape[1]

    def pick(v, values):
        return sum(value * same(v, i) for i, value in enumerate(values))

    targets = [pick(z, [TARGETS[i][k] for i in range(n_lat)]) for k in range(n_lat - 1)]
    first = [pick(z, [FIRST[i][k] for i in range(n_lat)]) for k in range(n_lat)]
    second = [pick(z, [SECOND[i][k] for i in range(n_lat)]) for k in range(n_lat)]

    def lay_peer(k):
        return {"lay": flip(l, k)}

    barrier = pltpu.get_barrier_semaphore()
    for k in range(n_lat - 1):
        pl.semaphore_signal(barrier, inc=1, device_id={"lat": targets[k]}, device_id_type=MESH)
    for k in reversed(range(1, n_lay)):
        pl.semaphore_signal(barrier, inc=1, device_id=lay_peer(k), device_id_type=MESH)

    load_acts = pltpu.make_async_copy(acts_hbm, acts_all.at[z], load.at[0])
    load_enc = pltpu.make_async_copy(wenc_hbm, wenc, load.at[1])
    load_dec = pltpu.make_async_copy(wdec_hbm, wdec, load.at[2])
    load_benc = pltpu.make_async_copy(benc_hbm, benc, load.at[3])
    load_bdec = pltpu.make_async_copy(bdec_hbm, bdec, load.at[4])
    load_acts.start()
    load_enc.start()
    load_dec.start()
    load_benc.start()
    load_bdec.start()

    pl.semaphore_wait(barrier, n_lat + n_lay - 2)

    def send(src, dst, send_sem, recv_sem, peer):
        pltpu.make_async_remote_copy(
            src_ref=src, dst_ref=dst, send_sem=send_sem, recv_sem=recv_sem,
            device_id=peer, device_id_type=MESH,
        ).start()

    def wait(view, sem):
        pltpu.make_async_copy(view, view, sem).wait()

    def to_lay(buf, k, sent, received):
        for j in sorted(range(1, n_lay), key=lambda j: (j < 2, j)):
            send(buf.at[k, 0], buf.at[k, j], sent, received.at[k], lay_peer(j))

    def total(buf, k, received):
        wait(buf.at[k, pl.ds(1, n_lay - 1)], received.at[k])
        whole = buf[k, l].astype(F32)
        for i in range(1, n_lay):
            whole += buf[k, flip(l, i)].astype(F32)
        return whole

    load_acts.wait()
    for k in range(n_lat - 1):
        send(acts_all.at[z], acts_all.at[z], acts_s, acts_r.at[z], {"lat": targets[k]})
    load_enc.wait()

    def encode(k):
        if k:
            wait(acts_all.at[first[k]], acts_r.at[first[k]])
        pre = jnp.dot(acts_all[first[k]], wenc[...], preferred_element_type=F32)
        pre_buf[k, 0] = pre.astype(BF16)
        to_lay(pre_buf, k, pre_s, pre_r)

    def decode(k):
        b = first[k]
        x = 4.0 * (total(pre_buf, k, pre_r) + benc[...].reshape(1, lat_dev))
        e = jnp.exp(-jnp.abs(x))
        code = (0.25 * (jnp.maximum(x, 0.0) + jnp.log1p(e))).astype(BF16)
        rec = jnp.dot(code, wdec[...], preferred_element_type=F32).astype(BF16)
        rec_mine[b] = rec
        owner = pick(b, OWNER)

        @pl.when(owner != z)
        def _():
            send(rec_mine.at[b], rec_buf.at[b, z], rec_s, rec_r.at[b], {"lat": owner})

        code_all[b] = code
        slope[b] = jnp.where(x >= 0.0, 1.0, e) / (1.0 + e)

    encode(0)
    load_dec.wait()
    wdec_t[...] = wdec[...].astype(F32).T.astype(BF16)
    for k in range(1, n_lat):
        encode(k)
    acts_t[...] = acts_all[...].reshape(rows, wide).astype(F32).T.astype(BF16)
    load_benc.wait()
    load_bdec.wait()
    for k in range(n_lat):
        decode(k)

    for i, owned in enumerate(OWNED):
        if owned:

            @pl.when(z == i)
            def _():
                for b in owned:
                    wait(rec_buf.at[b, pl.ds(0, n_lat - 1)], rec_r.at[b])
                    err = bdec[...] - acts_all[b].astype(F32) + rec_mine[b].astype(F32)
                    for j in SPREAD[i]:
                        err += rec_buf[b, j].astype(F32)
                    err_all[b] = err.astype(BF16)
                    for j in SPREAD[i]:
                        send(err_all.at[b], err_all.at[b], err_s, err_r.at[b], {"lat": j})

    code_t = code_all[...].reshape(rows, lat_dev).astype(F32).T.astype(BF16)
    for k in range(n_lat):
        b = second[k]

        @pl.when(pick(b, OWNER) != z)
        def _():
            wait(err_all.at[b], err_r.at[b])

        back = jnp.dot(err_all[b], wdec_t[...], preferred_element_type=F32)
        back_buf[k, 0] = back.astype(BF16)
        to_lay(back_buf, k, back_s, back_r)
    errs = err_all[...].reshape(rows, wide)
    dec_out[...] = jnp.dot(code_t, errs, preferred_element_type=F32).astype(BF16)
    for k in range(n_lat):
        b = second[k]
        lat_out[b] = (total(back_buf, k, back_r) * slope[b]).astype(BF16)

    wait(acts_all.at[pl.ds(0, n_lat - 1)], acts_s)
    wait(pre_buf.at[:, pl.ds(1, n_lay - 1)], pre_s)
    wait(back_buf.at[:, pl.ds(1, n_lay - 1)], back_s)
    for i, owned in enumerate(OWNED):

        @pl.when(z == i)
        def _():
            wait(rec_mine.at[pl.ds(0, n_lat - len(owned))], rec_s)
            if owned:
                wait(rec_buf.at[pl.ds(0, len(owned)), pl.ds(0, n_lat - 1)], err_s)


def finish(chunks, lat, acts_t, dec, lat_hbm, enc_hbm, dec_hbm, enc, sems):
    rows, lat_dev = lat.shape[0] * lat.shape[1], lat.shape[2]
    copies = [
        pltpu.make_async_copy(dec, dec_hbm, sems.at[0]),
        pltpu.make_async_copy(lat, lat_hbm, sems.at[1]),
    ]
    for copy in copies:
        copy.start()
    grad = lat[...].reshape(rows, lat_dev)
    tall = enc.shape[0] // chunks
    for c in range(chunks):
        cut = pl.ds(c * tall, tall)
        enc[cut] = jnp.dot(acts_t[cut], grad, preferred_element_type=F32).astype(BF16)
        copy = pltpu.make_async_copy(enc.at[cut], enc_hbm.at[cut], sems.at[2 + c])
        copy.start()
        copies.append(copy)
    for copy in copies:
        copy.wait()


def solution(mesh):
    n_lat, n_lay = mesh.shape["lat"], mesh.shape["lay"]

    def on_device(acts, w_enc, w_dec, b_enc, b_dec):
        row_dev, lay_dev, width = acts.shape
        lat_dev = w_enc.shape[2]
        wide, rows = lay_dev * width, n_lat * row_dev
        hbm = pl.BlockSpec(memory_space=pltpu.HBM)
        vmem = pl.BlockSpec(memory_space=pltpu.VMEM)
        dma = pltpu.SemaphoreType.DMA
        line = n_lat == len(OWNER) and n_lay & (n_lay - 1) == 0
        groups = 4 if n_lat & (n_lat - 1) == 0 and n_lat % 4 == 0 else 1
        if line:
            groups = n_lat
        part = rows // groups
        chunks = 5 if wide % 80 == 0 else 1
        out_shape = [
            pltpu.VMEM((groups, part, lat_dev), BF16),
            pltpu.VMEM((wide, rows), BF16),
            pltpu.VMEM((lat_dev, wide), BF16),
        ]
        rows_buf = pltpu.VMEM((n_lat, row_dev, wide), BF16)
        if line:
            kernel = functools.partial(line_step, n_lat, n_lay)
            in_specs = [hbm] * 5
            lay_buf = pltpu.VMEM((groups, n_lay, part, lat_dev), BF16)
            scratch = [
                rows_buf,
                pltpu.VMEM((wide, lat_dev), BF16),
                pltpu.VMEM((lat_dev, wide), BF16),
                pltpu.VMEM((wide, lat_dev), BF16),
                pltpu.VMEM((lat_dev,), F32),
                pltpu.VMEM((1, wide), F32),
                lay_buf,
                lay_buf,
                rows_buf,
                pltpu.VMEM((n_lat, n_lat, row_dev, wide), BF16),
                rows_buf,
                pltpu.VMEM((groups, part, lat_dev), BF16),
                pltpu.VMEM((groups, part, lat_dev), F32),
                dma((5,)),
                dma, dma((n_lat,)),
                dma, dma((groups,)),
                dma, dma((n_lat,)),
                dma, dma((n_lat,)),
                dma, dma((groups,)),
            ]
        else:
            kernel = functools.partial(step, n_lat, n_lay, groups)
            in_specs = [hbm, hbm, hbm, vmem, vmem]
            scratch = [
                rows_buf,
                pltpu.VMEM((wide, lat_dev), BF16),
                pltpu.VMEM((lat_dev, wide), BF16),
                pltpu.VMEM((wide, lat_dev), BF16),
                pltpu.VMEM((n_lay, groups, part, lat_dev), BF16),
                pltpu.VMEM((n_lay, groups, part, lat_dev), BF16),
                rows_buf,
                rows_buf,
                rows_buf,
                pltpu.VMEM((groups, part, lat_dev), BF16),
                pltpu.VMEM((groups, part, lat_dev), F32),
                dma((3,)),
                dma((n_lat,)), dma((n_lat,)),
                dma((groups, n_lay)), dma((groups, n_lay)),
                dma((n_lat,)), dma((n_lat,)),
                dma((n_lat,)), dma((n_lat,)),
                dma((groups, n_lay)), dma((groups, n_lay)),
            ]
        lat_part, acts_t, dec_part = pl.pallas_call(
            kernel,
            out_shape=out_shape,
            in_specs=in_specs,
            out_specs=[vmem, vmem, vmem],
            scratch_shapes=scratch,
            compiler_params=pltpu.CompilerParams(collective_id=0, has_side_effects=True),
            cost_estimate=pl.CostEstimate(
                flops=8 * rows * wide * lat_dev,
                bytes_accessed=4 * wide * lat_dev,
                transcendentals=0,
            ),
        )(
            acts.reshape(row_dev, wide),
            w_enc.reshape(wide, lat_dev),
            w_dec.reshape(lat_dev, wide),
            b_enc,
            b_dec.reshape(1, wide),
        )
        lat_grad, enc_grad, dec_grad = pl.pallas_call(
            functools.partial(finish, chunks),
            out_shape=[
                jax.ShapeDtypeStruct((groups, part, lat_dev), BF16),
                jax.ShapeDtypeStruct((wide, lat_dev), BF16),
                jax.ShapeDtypeStruct((lat_dev, wide), BF16),
            ],
            in_specs=[vmem, vmem, vmem],
            out_specs=[hbm, hbm, hbm],
            scratch_shapes=[pltpu.VMEM((wide, lat_dev), BF16), dma((2 + chunks,))],
            compiler_params=pltpu.CompilerParams(vmem_limit_bytes=8 * wide * lat_dev),
            cost_estimate=pl.CostEstimate(
                flops=2 * rows * wide * lat_dev,
                bytes_accessed=4 * wide * lat_dev,
                transcendentals=0,
            ),
        )(lat_part, acts_t, dec_part)
        return (
            lat_grad.reshape(rows, lat_dev),
            enc_grad.reshape(lay_dev, width, lat_dev),
            dec_grad.reshape(lat_dev, lay_dev, width),
        )

    in_specs = (
        P(("grp", "lat"), "lay", None),
        P("lay", None, "lat"),
        P("lat", "lay", None),
        P("lat"),
        P("lay", None),
    )
    out_specs = (P("grp", "lat"), P(("grp", "lay"), None, "lat"), P("lat", ("grp", "lay"), None))
    return jax.shard_map(
        on_device, mesh=mesh, in_specs=in_specs, out_specs=out_specs, check_vma=False
    )
```

```python
import functools

import jax
import jax.numpy as jnp
from jax import lax
from jax.experimental import pallas as pl
from jax.experimental.pallas import tpu as pltpu
from jax.sharding import PartitionSpec as P

MESH = pl.DeviceIdType.MESH
F32, BF16 = jnp.float32, jnp.bfloat16


def flip(v, j):
    out, bit = v, 1
    while bit <= j:
        if j & bit:
            out = out + bit * (1 - 2 * lax.rem(lax.div(v, bit), 2))
        bit *= 2
    return out


def step(
    n_lat, n_lay, groups, acts_hbm, wenc_hbm, wdec_hbm, benc_ref, bdec_ref,
    lat_out, acts_t, dec_out,
    acts_all, wenc, wdec, wdec_t, pre_buf, back_buf, rec_mine, rec_buf, err_all, code_all, slope,
    load, acts_s, acts_r, pre_s, pre_r, rec_s, rec_r, err_s, err_r, back_s, back_r,
):
    z, l = lax.axis_index("lat"), lax.axis_index("lay")
    row_dev, wide = acts_all.shape[1:]
    rows, lat_dev = n_lat * row_dev, wenc.shape[1]
    size = n_lat // groups
    part = size * row_dev

    load_acts = pltpu.make_async_copy(acts_hbm, acts_all.at[z], load.at[0])
    load_enc = pltpu.make_async_copy(wenc_hbm, wenc, load.at[1])
    load_dec = pltpu.make_async_copy(wdec_hbm, wdec, load.at[2])
    load_acts.start()
    load_enc.start()
    load_dec.start()

    if groups > 1:
        dest = source = lambda j: flip(z, j)
    else:
        dest = lambda j: lax.rem(z + j, n_lat)
        source = lambda j: lax.rem(z + n_lat - j, n_lat)
    group = [flip(lax.div(z, size), g) if groups > 1 else 0 for g in range(groups)]

    def lay_peer(k):
        return {"lay": lax.rem(l + k, n_lay)}

    barrier = pltpu.get_barrier_semaphore()
    for j in reversed(range(1, n_lat)):
        pl.semaphore_signal(
            barrier, inc=1, device_id={"lat": dest(j)}, device_id_type=MESH
        )
    for k in range(1, n_lay):
        pl.semaphore_signal(barrier, inc=1, device_id=lay_peer(k), device_id_type=MESH)
    pl.semaphore_wait(barrier, n_lat + n_lay - 2)

    started = []

    def send(src, dst, send_sem, recv_sem, peer):
        copy = pltpu.make_async_remote_copy(
            src_ref=src, dst_ref=dst, send_sem=send_sem, recv_sem=recv_sem,
            device_id=peer, device_id_type=MESH,
        )
        copy.start()
        started.append(copy)
        return copy

    def to_lat(buf, sent, received):
        return {
            j: send(buf.at[z], buf.at[z], sent.at[j], received.at[j], {"lat": dest(j)})
            for j in range(1, n_lat)
        }

    def to_lay(buf, g, sent, received):
        block = buf.at[l, group[g]]
        return [
            send(block, block, sent.at[g, k], received.at[g, k], lay_peer(k))
            for k in range(1, n_lay)
        ]

    def arrive(copies, g):
        for j in range(g * size, (g + 1) * size):
            if j:
                copies[j].wait_recv()

    def rows_of(buf, g):
        return buf[pl.ds(group[g] * size, size)].reshape(part, wide)

    def total(buf, g):
        whole = buf[0, group[g]].astype(F32)
        for i in range(1, n_lay):
            whole += buf[i, group[g]].astype(F32)
        return whole

    load_acts.wait()
    acts_copies = to_lat(acts_all, acts_s, acts_r)
    load_enc.wait()
    pre_copies, rec_copies = {}, {}

    def encode(g):
        arrive(acts_copies, g)
        pre = jnp.dot(rows_of(acts_all, g), wenc[...], preferred_element_type=F32)
        pre_buf[l, group[g]] = pre.astype(BF16)
        pre_copies[g] = to_lay(pre_buf, g, pre_s, pre_r)

    def decode(g):
        for copy in pre_copies[g]:
            copy.wait_recv()
        x = 4.0 * (total(pre_buf, g) + benc_ref[...].reshape(1, lat_dev))
        e = jnp.exp(-jnp.abs(x))
        code = (0.25 * (jnp.maximum(x, 0.0) + jnp.log1p(e))).astype(BF16)
        rec = jnp.dot(code, wdec[...], preferred_element_type=F32).astype(BF16)
        rec_mine[pl.ds(group[g] * size, size)] = rec.reshape(size, row_dev, wide)
        for j in range(g * size, (g + 1) * size):
            if j:
                rec_copies[j] = send(
                    rec_mine.at[dest(j)], rec_buf.at[z], rec_s.at[j], rec_r.at[j],
                    {"lat": dest(j)},
                )
        code_all[group[g]] = code
        slope[group[g]] = jnp.where(x >= 0.0, 1.0, e) / (1.0 + e)

    for g in range(groups):
        encode(g)
        if g == 0:
            load_dec.wait()
    for g in [*range(1, groups), 0]:
        decode(g)
    wdec_t[...] = wdec[...].astype(F32).T.astype(BF16)
    acts_t[...] = acts_all[...].reshape(rows, wide).astype(F32).T.astype(BF16)
    code_t = code_all[...].reshape(rows, lat_dev).astype(F32).T.astype(BF16)
    err = bdec_ref[...] - acts_all[z].astype(F32) + rec_mine[z].astype(F32)
    for j in range(1, n_lat):
        rec_copies[j].wait_recv()
        err += rec_buf[source(j)].astype(F32)
    err_all[z] = err.astype(BF16)
    err_copies = to_lat(err_all, err_s, err_r)
    back_copies = {}
    for g in range(groups):
        arrive(err_copies, g)
        back = jnp.dot(rows_of(err_all, g), wdec_t[...], preferred_element_type=F32)
        back_buf[l, group[g]] = back.astype(BF16)
        back_copies[g] = to_lay(back_buf, g, back_s, back_r)
    errs = err_all[...].reshape(rows, wide)
    dec_out[...] = jnp.dot(code_t, errs, preferred_element_type=F32).astype(BF16)
    for g in range(groups):
        for copy in back_copies[g]:
            copy.wait_recv()
        lat_out[group[g]] = (total(back_buf, g) * slope[group[g]]).astype(BF16)
    for copy in started:
        copy.wait_send()


def same(v, c):
    return lax.div(1, 1 + (v - c) * (v - c))


OWNER = [2, 2, 1, 0]
FIRST = [[0, 1, 2, 3], [1, 2, 3, 0], [2, 3, 1, 0], [3, 2, 1, 0]]
SECOND = [[3, 1, 2, 0], [2, 3, 1, 0], [0, 1, 2, 3], [1, 0, 2, 3]]
OWNED = [[3], [2], [1, 0], []]
TARGETS = [[3, 2, 1], [3, 2, 0], [0, 1, 3], [0, 1, 2]]
SPREAD = [[0, 1, 2, 3], [0, 3, 2, 1], [0, 3, 2], []]
LATER = [[], [], [(1, 1), (0, 1)], []]


def line_step(
    n_lat, n_lay, acts_hbm, wenc_hbm, wdec_hbm, benc_hbm, bdec_hbm,
    lat_out, acts_t, dec_out,
    acts_all, wenc, wdec, wdec_t, benc, bdec, pre_buf, back_buf, rec_mine, rec_buf, err_mine, err_all,
    code_all, slope,
    load, acts_s, acts_r, pre_s, pre_r, rec_s, rec_r, err_s, err_r, back_s, back_r,
):
    z, l = lax.axis_index("lat"), lax.axis_index("lay")
    row_dev, wide = acts_all.shape[1:]
    rows, lat_dev = n_lat * row_dev, wenc.shape[1]

    def pick(v, values):
        return sum(value * same(v, i) for i, value in enumerate(values))

    targets = [pick(z, [TARGETS[i][k] for i in range(n_lat)]) for k in range(n_lat - 1)]
    first = [pick(z, [FIRST[i][k] for i in range(n_lat)]) for k in range(n_lat)]
    second = [pick(z, [SECOND[i][k] for i in range(n_lat)]) for k in range(n_lat)]

    def lay_peer(k):
        return {"lay": flip(l, k)}

    barrier = pltpu.get_barrier_semaphore()
    for k in range(n_lat - 1):
        pl.semaphore_signal(barrier, inc=1, device_id={"lat": targets[k]}, device_id_type=MESH)
    for k in reversed(range(1, n_lay)):
        pl.semaphore_signal(barrier, inc=1, device_id=lay_peer(k), device_id_type=MESH)

    load_acts = pltpu.make_async_copy(acts_hbm, acts_all.at[z], load.at[0])
    load_enc = pltpu.make_async_copy(wenc_hbm, wenc, load.at[1])
    load_dec = pltpu.make_async_copy(wdec_hbm, wdec, load.at[2])
    load_benc = pltpu.make_async_copy(benc_hbm, benc, load.at[3])
    load_bdec = pltpu.make_async_copy(bdec_hbm, bdec, load.at[4])
    load_acts.start()
    load_enc.start()
    load_dec.start()
    load_benc.start()
    load_bdec.start()

    pl.semaphore_wait(barrier, n_lat + n_lay - 2)

    def send(src, dst, send_sem, recv_sem, peer):
        pltpu.make_async_remote_copy(
            src_ref=src, dst_ref=dst, send_sem=send_sem, recv_sem=recv_sem,
            device_id=peer, device_id_type=MESH,
        ).start()

    def wait(view, sem):
        pltpu.make_async_copy(view, view, sem).wait()

    def to_lay(buf, k, sent, received):
        for j in sorted(range(1, n_lay), key=lambda j: (j < 2, j)):
            send(buf.at[k, 0], buf.at[k, j], sent, received.at[k], lay_peer(j))

    def total(buf, k, received):
        wait(buf.at[k, pl.ds(1, n_lay - 1)], received.at[k])
        whole = buf[k, l].astype(F32)
        for i in range(1, n_lay):
            whole += buf[k, flip(l, i)].astype(F32)
        return whole

    load_acts.wait()
    for k in range(n_lat - 1):
        send(acts_all.at[z], acts_all.at[z], acts_s, acts_r.at[z], {"lat": targets[k]})
    load_enc.wait()

    def encode(k):
        if k:
            wait(acts_all.at[first[k]], acts_r.at[first[k]])
        pre = jnp.dot(acts_all[first[k]], wenc[...], preferred_element_type=F32)
        pre_buf[k, 0] = pre.astype(BF16)
        to_lay(pre_buf, k, pre_s, pre_r)

    def decode(k):
        b = first[k]
        x = 4.0 * (total(pre_buf, k, pre_r) + benc[...].reshape(1, lat_dev))
        e = jnp.exp(-jnp.abs(x))
        code = (0.25 * (jnp.maximum(x, 0.0) + jnp.log1p(e))).astype(BF16)
        rec = jnp.dot(code, wdec[...], preferred_element_type=F32)
        owner = pick(b, OWNER)
        base = bdec[...] - acts_all[b].astype(F32)
        rec_mine[b] = (rec + jnp.where(owner == z, base, 0.0)).astype(BF16)
        peer = {"lat": owner, "lay": flip(l, 1)}
        send(rec_mine.at[b], rec_buf.at[b, z], rec_s, rec_r.at[b], peer)

        code_all[b] = code
        slope[b] = jnp.where(x >= 0.0, 1.0, e) / (1.0 + e)

    encode(0)
    load_dec.wait()
    wdec_t[...] = wdec[...].astype(F32).T.astype(BF16)
    for k in range(1, n_lat):
        encode(k)
    acts_t[...] = acts_all[...].reshape(rows, wide).astype(F32).T.astype(BF16)
    load_benc.wait()
    load_bdec.wait()
    for k in range(n_lat):
        decode(k)

    for i, owned in enumerate(OWNED):
        if owned:

            @pl.when(z == i)
            def _():
                for b in owned:
                    wait(rec_buf.at[b], rec_r.at[b])
                    err = rec_buf[b, 0].astype(F32)
                    for j in range(1, n_lat):
                        err += rec_buf[b, j].astype(F32)
                    err_mine[b] = err.astype(BF16)
                    for j in SPREAD[i]:
                        peer = {"lat": j, "lay": flip(l, 1)}
                        send(err_mine.at[b], err_all.at[b], err_s, err_r.at[b], peer)
                for b, j in LATER[i]:
                    peer = {"lat": j, "lay": flip(l, 1)}
                    send(err_mine.at[b], err_all.at[b], err_s, err_r.at[b], peer)

    code_t = code_all[...].reshape(rows, lat_dev).astype(F32).T.astype(BF16)
    for k in range(n_lat):
        b = second[k]
        wait(err_all.at[b], err_r.at[b])
        back = jnp.dot(err_all[b], wdec_t[...], preferred_element_type=F32)
        back_buf[k, 0] = back.astype(BF16)
        to_lay(back_buf, k, back_s, back_r)
    errs = err_all[...].reshape(rows, wide)
    dec_out[...] = jnp.dot(code_t, errs, preferred_element_type=F32).astype(BF16)
    for k in range(n_lat):
        b = second[k]
        lat_out[b] = (total(back_buf, k, back_r) * slope[b]).astype(BF16)

    wait(acts_all.at[pl.ds(0, n_lat - 1)], acts_s)
    wait(pre_buf.at[:, pl.ds(1, n_lay - 1)], pre_s)
    wait(back_buf.at[:, pl.ds(1, n_lay - 1)], back_s)
    wait(rec_mine, rec_s)
    for i, owned in enumerate(OWNED):
        if owned:

            @pl.when(z == i)
            def _():
                wait(rec_buf.at[pl.ds(0, len(owned))], err_s)


def finish(chunks, lat, acts_t, dec, lat_hbm, enc_hbm, dec_hbm, enc, sems):
    rows, lat_dev = lat.shape[0] * lat.shape[1], lat.shape[2]
    copies = [
        pltpu.make_async_copy(dec, dec_hbm, sems.at[0]),
        pltpu.make_async_copy(lat, lat_hbm, sems.at[1]),
    ]
    for copy in copies:
        copy.start()
    grad = lat[...].reshape(rows, lat_dev)
    tall = enc.shape[0] // chunks
    for c in range(chunks):
        cut = pl.ds(c * tall, tall)
        enc[cut] = jnp.dot(acts_t[cut], grad, preferred_element_type=F32).astype(BF16)
        copy = pltpu.make_async_copy(enc.at[cut], enc_hbm.at[cut], sems.at[2 + c])
        copy.start()
        copies.append(copy)
    for copy in copies:
        copy.wait()


def solution(mesh):
    n_lat, n_lay = mesh.shape["lat"], mesh.shape["lay"]

    def on_device(acts, w_enc, w_dec, b_enc, b_dec):
        row_dev, lay_dev, width = acts.shape
        lat_dev = w_enc.shape[2]
        wide, rows = lay_dev * width, n_lat * row_dev
        hbm = pl.BlockSpec(memory_space=pltpu.HBM)
        vmem = pl.BlockSpec(memory_space=pltpu.VMEM)
        dma = pltpu.SemaphoreType.DMA
        line = n_lat == len(OWNER) and n_lay & (n_lay - 1) == 0 and n_lay > 1
        groups = 4 if n_lat & (n_lat - 1) == 0 and n_lat % 4 == 0 else 1
        if line:
            groups = n_lat
        part = rows // groups
        chunks = 5 if wide % 80 == 0 else 1
        out_shape = [
            pltpu.VMEM((groups, part, lat_dev), BF16),
            pltpu.VMEM((wide, rows), BF16),
            pltpu.VMEM((lat_dev, wide), BF16),
        ]
        rows_buf = pltpu.VMEM((n_lat, row_dev, wide), BF16)
        if line:
            kernel = functools.partial(line_step, n_lat, n_lay)
            in_specs = [hbm] * 5
            lay_buf = pltpu.VMEM((groups, n_lay, part, lat_dev), BF16)
            scratch = [
                rows_buf,
                pltpu.VMEM((wide, lat_dev), BF16),
                pltpu.VMEM((lat_dev, wide), BF16),
                pltpu.VMEM((wide, lat_dev), BF16),
                pltpu.VMEM((lat_dev,), F32),
                pltpu.VMEM((1, wide), F32),
                lay_buf,
                lay_buf,
                rows_buf,
                pltpu.VMEM((n_lat, n_lat, row_dev, wide), BF16),
                rows_buf,
                rows_buf,
                pltpu.VMEM((groups, part, lat_dev), BF16),
                pltpu.VMEM((groups, part, lat_dev), F32),
                dma((5,)),
                dma, dma((n_lat,)),
                dma, dma((groups,)),
                dma, dma((n_lat,)),
                dma, dma((n_lat,)),
                dma, dma((groups,)),
            ]
        else:
            kernel = functools.partial(step, n_lat, n_lay, groups)
            in_specs = [hbm, hbm, hbm, vmem, vmem]
            scratch = [
                rows_buf,
                pltpu.VMEM((wide, lat_dev), BF16),
                pltpu.VMEM((lat_dev, wide), BF16),
                pltpu.VMEM((wide, lat_dev), BF16),
                pltpu.VMEM((n_lay, groups, part, lat_dev), BF16),
                pltpu.VMEM((n_lay, groups, part, lat_dev), BF16),
                rows_buf,
                rows_buf,
                rows_buf,
                pltpu.VMEM((groups, part, lat_dev), BF16),
                pltpu.VMEM((groups, part, lat_dev), F32),
                dma((3,)),
                dma((n_lat,)), dma((n_lat,)),
                dma((groups, n_lay)), dma((groups, n_lay)),
                dma((n_lat,)), dma((n_lat,)),
                dma((n_lat,)), dma((n_lat,)),
                dma((groups, n_lay)), dma((groups, n_lay)),
            ]
        lat_part, acts_t, dec_part = pl.pallas_call(
            kernel,
            out_shape=out_shape,
            in_specs=in_specs,
            out_specs=[vmem, vmem, vmem],
            scratch_shapes=scratch,
            compiler_params=pltpu.CompilerParams(collective_id=0, has_side_effects=True),
            cost_estimate=pl.CostEstimate(
                flops=8 * rows * wide * lat_dev,
                bytes_accessed=4 * wide * lat_dev,
                transcendentals=0,
            ),
        )(
            acts.reshape(row_dev, wide),
            w_enc.reshape(wide, lat_dev),
            w_dec.reshape(lat_dev, wide),
            b_enc,
            b_dec.reshape(1, wide),
        )
        lat_grad, enc_grad, dec_grad = pl.pallas_call(
            functools.partial(finish, chunks),
            out_shape=[
                jax.ShapeDtypeStruct((groups, part, lat_dev), BF16),
                jax.ShapeDtypeStruct((wide, lat_dev), BF16),
                jax.ShapeDtypeStruct((lat_dev, wide), BF16),
            ],
            in_specs=[vmem, vmem, vmem],
            out_specs=[hbm, hbm, hbm],
            scratch_shapes=[pltpu.VMEM((wide, lat_dev), BF16), dma((2 + chunks,))],
            compiler_params=pltpu.CompilerParams(vmem_limit_bytes=8 * wide * lat_dev),
            cost_estimate=pl.CostEstimate(
                flops=2 * rows * wide * lat_dev,
                bytes_accessed=4 * wide * lat_dev,
                transcendentals=0,
            ),
        )(lat_part, acts_t, dec_part)
        return (
            lat_grad.reshape(rows, lat_dev),
            enc_grad.reshape(lay_dev, width, lat_dev),
            dec_grad.reshape(lat_dev, lay_dev, width),
        )

    in_specs = (
        P(("grp", "lat"), "lay", None),
        P("lay", None, "lat"),
        P("lat", "lay", None),
        P("lat"),
        P("lay", None),
    )
    out_specs = (P("grp", "lat"), P(("grp", "lay"), None, "lat"), P("lat", ("grp", "lay"), None))
    return jax.shard_map(
        on_device, mesh=mesh, in_specs=in_specs, out_specs=out_specs, check_vma=False
    )
```

```python
import functools

import jax
import jax.numpy as jnp
from jax import lax
from jax.experimental import pallas as pl
from jax.experimental.pallas import tpu as pltpu
from jax.sharding import PartitionSpec as P

MESH = pl.DeviceIdType.MESH
F32, BF16 = jnp.float32, jnp.bfloat16


def flip(v, j):
    out, bit = v, 1
    while bit <= j:
        if j & bit:
            out = out + bit * (1 - 2 * lax.rem(lax.div(v, bit), 2))
        bit *= 2
    return out


def step(
    n_lat, n_lay, groups, acts_hbm, wenc_hbm, wdec_hbm, benc_ref, bdec_ref,
    lat_out, acts_t, dec_out,
    acts_all, wenc, wdec, wdec_t, pre_buf, back_buf, rec_mine, rec_buf, err_all, code_all, slope,
    load, acts_s, acts_r, pre_s, pre_r, rec_s, rec_r, err_s, err_r, back_s, back_r,
):
    z, l = lax.axis_index("lat"), lax.axis_index("lay")
    row_dev, wide = acts_all.shape[1:]
    rows, lat_dev = n_lat * row_dev, wenc.shape[1]
    size = n_lat // groups
    part = size * row_dev

    load_acts = pltpu.make_async_copy(acts_hbm, acts_all.at[z], load.at[0])
    load_enc = pltpu.make_async_copy(wenc_hbm, wenc, load.at[1])
    load_dec = pltpu.make_async_copy(wdec_hbm, wdec, load.at[2])
    load_acts.start()
    load_enc.start()
    load_dec.start()

    if groups > 1:
        dest = source = lambda j: flip(z, j)
    else:
        dest = lambda j: lax.rem(z + j, n_lat)
        source = lambda j: lax.rem(z + n_lat - j, n_lat)
    group = [flip(lax.div(z, size), g) if groups > 1 else 0 for g in range(groups)]

    def lay_peer(k):
        return {"lay": lax.rem(l + k, n_lay)}

    barrier = pltpu.get_barrier_semaphore()
    for j in reversed(range(1, n_lat)):
        pl.semaphore_signal(
            barrier, inc=1, device_id={"lat": dest(j)}, device_id_type=MESH
        )
    for k in range(1, n_lay):
        pl.semaphore_signal(barrier, inc=1, device_id=lay_peer(k), device_id_type=MESH)
    pl.semaphore_wait(barrier, n_lat + n_lay - 2)

    started = []

    def send(src, dst, send_sem, recv_sem, peer):
        copy = pltpu.make_async_remote_copy(
            src_ref=src, dst_ref=dst, send_sem=send_sem, recv_sem=recv_sem,
            device_id=peer, device_id_type=MESH,
        )
        copy.start()
        started.append(copy)
        return copy

    def to_lat(buf, sent, received):
        return {
            j: send(buf.at[z], buf.at[z], sent.at[j], received.at[j], {"lat": dest(j)})
            for j in range(1, n_lat)
        }

    def to_lay(buf, g, sent, received):
        block = buf.at[l, group[g]]
        return [
            send(block, block, sent.at[g, k], received.at[g, k], lay_peer(k))
            for k in range(1, n_lay)
        ]

    def arrive(copies, g):
        for j in range(g * size, (g + 1) * size):
            if j:
                copies[j].wait_recv()

    def rows_of(buf, g):
        return buf[pl.ds(group[g] * size, size)].reshape(part, wide)

    def total(buf, g):
        whole = buf[0, group[g]].astype(F32)
        for i in range(1, n_lay):
            whole += buf[i, group[g]].astype(F32)
        return whole

    load_acts.wait()
    acts_copies = to_lat(acts_all, acts_s, acts_r)
    load_enc.wait()
    pre_copies, rec_copies = {}, {}

    def encode(g):
        arrive(acts_copies, g)
        pre = jnp.dot(rows_of(acts_all, g), wenc[...], preferred_element_type=F32)
        pre_buf[l, group[g]] = pre.astype(BF16)
        pre_copies[g] = to_lay(pre_buf, g, pre_s, pre_r)

    def decode(g):
        for copy in pre_copies[g]:
            copy.wait_recv()
        x = 4.0 * (total(pre_buf, g) + benc_ref[...].reshape(1, lat_dev))
        e = jnp.exp(-jnp.abs(x))
        code = (0.25 * (jnp.maximum(x, 0.0) + jnp.log1p(e))).astype(BF16)
        rec = jnp.dot(code, wdec[...], preferred_element_type=F32).astype(BF16)
        rec_mine[pl.ds(group[g] * size, size)] = rec.reshape(size, row_dev, wide)
        for j in range(g * size, (g + 1) * size):
            if j:
                rec_copies[j] = send(
                    rec_mine.at[dest(j)], rec_buf.at[z], rec_s.at[j], rec_r.at[j],
                    {"lat": dest(j)},
                )
        code_all[group[g]] = code
        slope[group[g]] = jnp.where(x >= 0.0, 1.0, e) / (1.0 + e)

    for g in range(groups):
        encode(g)
        if g == 0:
            load_dec.wait()
    for g in [*range(1, groups), 0]:
        decode(g)
    wdec_t[...] = wdec[...].astype(F32).T.astype(BF16)
    acts_t[...] = acts_all[...].reshape(rows, wide).astype(F32).T.astype(BF16)
    code_t = code_all[...].reshape(rows, lat_dev).astype(F32).T.astype(BF16)
    err = bdec_ref[...] - acts_all[z].astype(F32) + rec_mine[z].astype(F32)
    for j in range(1, n_lat):
        rec_copies[j].wait_recv()
        err += rec_buf[source(j)].astype(F32)
    err_all[z] = err.astype(BF16)
    err_copies = to_lat(err_all, err_s, err_r)
    back_copies = {}
    for g in range(groups):
        arrive(err_copies, g)
        back = jnp.dot(rows_of(err_all, g), wdec_t[...], preferred_element_type=F32)
        back_buf[l, group[g]] = back.astype(BF16)
        back_copies[g] = to_lay(back_buf, g, back_s, back_r)
    errs = err_all[...].reshape(rows, wide)
    dec_out[...] = jnp.dot(code_t, errs, preferred_element_type=F32).astype(BF16)
    for g in range(groups):
        for copy in back_copies[g]:
            copy.wait_recv()
        lat_out[group[g]] = (total(back_buf, g) * slope[group[g]]).astype(BF16)
    for copy in started:
        copy.wait_send()


def same(v, c):
    return lax.div(1, 1 + (v - c) * (v - c))


OWNER = [2, 2, 1, 0]
FIRST = [[0, 1, 2, 3], [1, 2, 3, 0], [2, 3, 1, 0], [3, 2, 1, 0]]
SECOND = [[3, 1, 2, 0], [2, 3, 1, 0], [0, 1, 2, 3], [1, 0, 2, 3]]
OWNED = [[3], [2], [1, 0], []]
TARGETS = [[3, 2, 1], [3, 2, 0], [0, 1, 3], [0, 1, 2]]
SPREAD = [[0, 1, 2, 3], [0, 3, 2, 1], [0, 3, 2], []]
LATER = [[], [], [(1, 1), (0, 1)], []]


def line_step(
    n_lat, n_lay, acts_hbm, wenc_hbm, wdec_hbm, benc_hbm, bdec_hbm,
    lat_out, acts_t, dec_out,
    acts_all, wenc, wdec, wdec_t, benc, bdec, pre_buf, back_buf, rec_mine, rec_buf, err_mine, err_all,
    code_all, slope,
    load, acts_s, acts_r, pre_s, pre_r, rec_s, rec_r, err_s, err_r, back_s, back_r,
):
    z, l = lax.axis_index("lat"), lax.axis_index("lay")
    row_dev, wide = acts_all.shape[1:]
    rows, lat_dev = n_lat * row_dev, wenc.shape[1]

    def pick(v, values):
        return sum(value * same(v, i) for i, value in enumerate(values))

    targets = [pick(z, [TARGETS[i][k] for i in range(n_lat)]) for k in range(n_lat - 1)]
    first = [pick(z, [FIRST[i][k] for i in range(n_lat)]) for k in range(n_lat)]
    second = [pick(z, [SECOND[i][k] for i in range(n_lat)]) for k in range(n_lat)]

    def lay_peer(k):
        return {"lay": flip(l, k)}

    odd = lax.rem(l, 2)
    barrier = pltpu.get_barrier_semaphore()
    for k in range(n_lat - 1):
        pl.semaphore_signal(barrier, inc=1, device_id={"lat": targets[k]}, device_id_type=MESH)
    for k in reversed(range(1, n_lay)):
        pl.semaphore_signal(barrier, inc=1, device_id=lay_peer(k), device_id_type=MESH)

    load_acts = pltpu.make_async_copy(acts_hbm, acts_all.at[z], load.at[0])
    load_enc = pltpu.make_async_copy(wenc_hbm, wenc, load.at[1])
    load_dec = pltpu.make_async_copy(wdec_hbm, wdec, load.at[2])
    load_benc = pltpu.make_async_copy(benc_hbm, benc, load.at[3])
    load_bdec = pltpu.make_async_copy(bdec_hbm, bdec, load.at[4])
    load_acts.start()
    load_enc.start()
    load_dec.start()
    load_benc.start()
    load_bdec.start()

    pl.semaphore_wait(barrier, n_lat + n_lay - 2)

    def send(src, dst, send_sem, recv_sem, peer):
        pltpu.make_async_remote_copy(
            src_ref=src, dst_ref=dst, send_sem=send_sem, recv_sem=recv_sem,
            device_id=peer, device_id_type=MESH,
        ).start()

    def wait(view, sem):
        pltpu.make_async_copy(view, view, sem).wait()

    def to_lay(buf, k, sent, received):
        for j in (2, 3):
            slot = j + odd * (5 - 2 * j)
            peer = flip(l, j) + odd * (flip(l, 5 - j) - flip(l, j))
            send(buf.at[k, 0], buf.at[k, slot], sent, received.at[k], {"lay": peer})
        send(buf.at[k, 0], buf.at[k, 1], sent, received.at[k], lay_peer(1))

    def total(buf, k, received):
        wait(buf.at[k, pl.ds(1, n_lay - 1)], received.at[k])
        whole = buf[k, l].astype(F32)
        for i in range(1, n_lay):
            whole += buf[k, flip(l, i)].astype(F32)
        return whole

    load_acts.wait()
    for k in range(n_lat - 1):
        send(acts_all.at[z], acts_all.at[z], acts_s, acts_r.at[z], {"lat": targets[k]})
    load_enc.wait()

    def encode(k):
        if k:
            wait(acts_all.at[first[k]], acts_r.at[first[k]])
        pre = jnp.dot(acts_all[first[k]], wenc[...], preferred_element_type=F32)
        pre_buf[k, 0] = pre.astype(BF16)
        to_lay(pre_buf, k, pre_s, pre_r)

    def decode(k):
        b = first[k]
        x = 4.0 * (total(pre_buf, k, pre_r) + benc[...].reshape(1, lat_dev))
        e = jnp.exp(-jnp.abs(x))
        code = (0.25 * (jnp.maximum(x, 0.0) + jnp.log1p(e))).astype(BF16)
        rec = jnp.dot(code, wdec[...], preferred_element_type=F32)
        owner = pick(b, OWNER)
        base = bdec[...] - acts_all[b].astype(F32)
        rec_mine[b] = (rec + jnp.where(owner == z, base, 0.0)).astype(BF16)
        peer = {"lat": owner, "lay": flip(l, 1)}
        send(rec_mine.at[b], rec_buf.at[b, z], rec_s, rec_r.at[b], peer)
        code_all[b] = code
        slope[b] = jnp.where(x >= 0.0, 1.0, e) / (1.0 + e)

    encode(0)
    load_dec.wait()
    wdec_t[...] = wdec[...].astype(F32).T.astype(BF16)
    for k in range(1, n_lat):
        encode(k)
    acts_t[...] = acts_all[...].reshape(rows, wide).astype(F32).T.astype(BF16)
    load_benc.wait()
    load_bdec.wait()
    for k in range(n_lat):
        decode(k)

    for i, owned in enumerate(OWNED):
        if owned:

            @pl.when(z == i)
            def _():
                for b in owned:
                    wait(rec_buf.at[b], rec_r.at[b])
                    err = rec_buf[b, 0].astype(F32)
                    for j in range(1, n_lat):
                        err += rec_buf[b, j].astype(F32)
                    err_mine[b] = err.astype(BF16)
                    for j in SPREAD[i]:
                        peer = {"lat": j, "lay": flip(l, 1)}
                        send(err_mine.at[b], err_all.at[b], err_s, err_r.at[b], peer)
                for b, j in LATER[i]:
                    peer = {"lat": j, "lay": flip(l, 1)}
                    send(err_mine.at[b], err_all.at[b], err_s, err_r.at[b], peer)

    code_t = code_all[...].reshape(rows, lat_dev).astype(F32).T.astype(BF16)
    for k in range(n_lat):
        b = second[k]
        wait(err_all.at[b], err_r.at[b])
        back = jnp.dot(err_all[b], wdec_t[...], preferred_element_type=F32)
        back_buf[k, 0] = back.astype(BF16)
        to_lay(back_buf, k, back_s, back_r)
    errs = err_all[...].reshape(rows, wide)
    dec_out[...] = jnp.dot(code_t, errs, preferred_element_type=F32).astype(BF16)
    for k in range(n_lat):
        b = second[k]
        lat_out[b] = (total(back_buf, k, back_r) * slope[b]).astype(BF16)

    wait(acts_all.at[pl.ds(0, n_lat - 1)], acts_s)
    wait(pre_buf.at[:, pl.ds(1, n_lay - 1)], pre_s)
    wait(back_buf.at[:, pl.ds(1, n_lay - 1)], back_s)
    wait(rec_mine, rec_s)
    for i, owned in enumerate(OWNED):
        if owned:

            @pl.when(z == i)
            def _():
                wait(rec_buf.at[pl.ds(0, len(owned))], err_s)


def finish(chunks, lat, acts_t, dec, lat_hbm, enc_hbm, dec_hbm, enc, sems):
    rows, lat_dev = lat.shape[0] * lat.shape[1], lat.shape[2]
    copies = [
        pltpu.make_async_copy(dec, dec_hbm, sems.at[0]),
        pltpu.make_async_copy(lat, lat_hbm, sems.at[1]),
    ]
    for copy in copies:
        copy.start()
    grad = lat[...].reshape(rows, lat_dev)
    tall = enc.shape[0] // chunks
    for c in range(chunks):
        cut = pl.ds(c * tall, tall)
        enc[cut] = jnp.dot(acts_t[cut], grad, preferred_element_type=F32).astype(BF16)
        copy = pltpu.make_async_copy(enc.at[cut], enc_hbm.at[cut], sems.at[2 + c])
        copy.start()
        copies.append(copy)
    for copy in copies:
        copy.wait()


def solution(mesh):
    n_lat, n_lay = mesh.shape["lat"], mesh.shape["lay"]

    def on_device(acts, w_enc, w_dec, b_enc, b_dec):
        row_dev, lay_dev, width = acts.shape
        lat_dev = w_enc.shape[2]
        wide, rows = lay_dev * width, n_lat * row_dev
        hbm = pl.BlockSpec(memory_space=pltpu.HBM)
        vmem = pl.BlockSpec(memory_space=pltpu.VMEM)
        dma = pltpu.SemaphoreType.DMA
        line = n_lat == len(OWNER) and n_lay == 4
        groups = 4 if n_lat & (n_lat - 1) == 0 and n_lat % 4 == 0 else 1
        if line:
            groups = n_lat
        part = rows // groups
        chunks = 5 if wide % 80 == 0 else 1
        out_shape = [
            pltpu.VMEM((groups, part, lat_dev), BF16),
            pltpu.VMEM((wide, rows), BF16),
            pltpu.VMEM((lat_dev, wide), BF16),
        ]
        rows_buf = pltpu.VMEM((n_lat, row_dev, wide), BF16)
        if line:
            kernel = functools.partial(line_step, n_lat, n_lay)
            in_specs = [hbm] * 5
            lay_buf = pltpu.VMEM((groups, n_lay, part, lat_dev), BF16)
            scratch = [
                rows_buf,
                pltpu.VMEM((wide, lat_dev), BF16),
                pltpu.VMEM((lat_dev, wide), BF16),
                pltpu.VMEM((wide, lat_dev), BF16),
                pltpu.VMEM((lat_dev,), F32),
                pltpu.VMEM((1, wide), F32),
                lay_buf,
                lay_buf,
                rows_buf,
                pltpu.VMEM((n_lat, n_lat, row_dev, wide), BF16),
                rows_buf,
                rows_buf,
                pltpu.VMEM((groups, part, lat_dev), BF16),
                pltpu.VMEM((groups, part, lat_dev), F32),
                dma((5,)),
                dma, dma((n_lat,)),
                dma, dma((groups,)),
                dma, dma((n_lat,)),
                dma, dma((n_lat,)),
                dma, dma((groups,)),
            ]
        else:
            kernel = functools.partial(step, n_lat, n_lay, groups)
            in_specs = [hbm, hbm, hbm, vmem, vmem]
            scratch = [
                rows_buf,
                pltpu.VMEM((wide, lat_dev), BF16),
                pltpu.VMEM((lat_dev, wide), BF16),
                pltpu.VMEM((wide, lat_dev), BF16),
                pltpu.VMEM((n_lay, groups, part, lat_dev), BF16),
                pltpu.VMEM((n_lay, groups, part, lat_dev), BF16),
                rows_buf,
                rows_buf,
                rows_buf,
                pltpu.VMEM((groups, part, lat_dev), BF16),
                pltpu.VMEM((groups, part, lat_dev), F32),
                dma((3,)),
                dma((n_lat,)), dma((n_lat,)),
                dma((groups, n_lay)), dma((groups, n_lay)),
                dma((n_lat,)), dma((n_lat,)),
                dma((n_lat,)), dma((n_lat,)),
                dma((groups, n_lay)), dma((groups, n_lay)),
            ]
        lat_part, acts_t, dec_part = pl.pallas_call(
            kernel,
            out_shape=out_shape,
            in_specs=in_specs,
            out_specs=[vmem, vmem, vmem],
            scratch_shapes=scratch,
            compiler_params=pltpu.CompilerParams(collective_id=0, has_side_effects=True),
            cost_estimate=pl.CostEstimate(
                flops=8 * rows * wide * lat_dev,
                bytes_accessed=4 * wide * lat_dev,
                transcendentals=0,
            ),
        )(
            acts.reshape(row_dev, wide),
            w_enc.reshape(wide, lat_dev),
            w_dec.reshape(lat_dev, wide),
            b_enc,
            b_dec.reshape(1, wide),
        )
        lat_grad, enc_grad, dec_grad = pl.pallas_call(
            functools.partial(finish, chunks),
            out_shape=[
                jax.ShapeDtypeStruct((groups, part, lat_dev), BF16),
                jax.ShapeDtypeStruct((wide, lat_dev), BF16),
                jax.ShapeDtypeStruct((lat_dev, wide), BF16),
            ],
            in_specs=[vmem, vmem, vmem],
            out_specs=[hbm, hbm, hbm],
            scratch_shapes=[pltpu.VMEM((wide, lat_dev), BF16), dma((2 + chunks,))],
            compiler_params=pltpu.CompilerParams(vmem_limit_bytes=8 * wide * lat_dev),
            cost_estimate=pl.CostEstimate(
                flops=2 * rows * wide * lat_dev,
                bytes_accessed=4 * wide * lat_dev,
                transcendentals=0,
            ),
        )(lat_part, acts_t, dec_part)
        return (
            lat_grad.reshape(rows, lat_dev),
            enc_grad.reshape(lay_dev, width, lat_dev),
            dec_grad.reshape(lat_dev, lay_dev, width),
        )

    in_specs = (
        P(("grp", "lat"), "lay", None),
        P("lay", None, "lat"),
        P("lat", "lay", None),
        P("lat"),
        P("lay", None),
    )
    out_specs = (P("grp", "lat"), P(("grp", "lay"), None, "lat"), P("lat", ("grp", "lay"), None))
    return jax.shard_map(
        on_device, mesh=mesh, in_specs=in_specs, out_specs=out_specs, check_vma=False
    )
```

```python
import functools

import jax
import jax.numpy as jnp
from jax import lax
from jax.experimental import pallas as pl
from jax.experimental.pallas import tpu as pltpu
from jax.sharding import PartitionSpec as P

MESH = pl.DeviceIdType.MESH
F32, BF16 = jnp.float32, jnp.bfloat16


def flip(v, j):
    out, bit = v, 1
    while bit <= j:
        if j & bit:
            out = out + bit * (1 - 2 * lax.rem(lax.div(v, bit), 2))
        bit *= 2
    return out


def step(
    n_lat, n_lay, groups, acts_hbm, wenc_hbm, wdec_hbm, benc_ref, bdec_ref,
    lat_out, acts_t, dec_out,
    acts_all, wenc, wdec, wdec_t, pre_buf, back_buf, rec_mine, rec_buf, err_all, code_all, slope,
    load, acts_s, acts_r, pre_s, pre_r, rec_s, rec_r, err_s, err_r, back_s, back_r,
):
    z, l = lax.axis_index("lat"), lax.axis_index("lay")
    row_dev, wide = acts_all.shape[1:]
    rows, lat_dev = n_lat * row_dev, wenc.shape[1]
    size = n_lat // groups
    part = size * row_dev

    load_acts = pltpu.make_async_copy(acts_hbm, acts_all.at[z], load.at[0])
    load_enc = pltpu.make_async_copy(wenc_hbm, wenc, load.at[1])
    load_dec = pltpu.make_async_copy(wdec_hbm, wdec, load.at[2])
    load_acts.start()
    load_enc.start()
    load_dec.start()

    if groups > 1:
        dest = source = lambda j: flip(z, j)
    else:
        dest = lambda j: lax.rem(z + j, n_lat)
        source = lambda j: lax.rem(z + n_lat - j, n_lat)
    group = [flip(lax.div(z, size), g) if groups > 1 else 0 for g in range(groups)]

    def lay_peer(k):
        return {"lay": lax.rem(l + k, n_lay)}

    barrier = pltpu.get_barrier_semaphore()
    for j in reversed(range(1, n_lat)):
        pl.semaphore_signal(
            barrier, inc=1, device_id={"lat": dest(j)}, device_id_type=MESH
        )
    for k in range(1, n_lay):
        pl.semaphore_signal(barrier, inc=1, device_id=lay_peer(k), device_id_type=MESH)
    pl.semaphore_wait(barrier, n_lat + n_lay - 2)

    started = []

    def send(src, dst, send_sem, recv_sem, peer):
        copy = pltpu.make_async_remote_copy(
            src_ref=src, dst_ref=dst, send_sem=send_sem, recv_sem=recv_sem,
            device_id=peer, device_id_type=MESH,
        )
        copy.start()
        started.append(copy)
        return copy

    def to_lat(buf, sent, received):
        return {
            j: send(buf.at[z], buf.at[z], sent.at[j], received.at[j], {"lat": dest(j)})
            for j in range(1, n_lat)
        }

    def to_lay(buf, g, sent, received):
        block = buf.at[l, group[g]]
        return [
            send(block, block, sent.at[g, k], received.at[g, k], lay_peer(k))
            for k in range(1, n_lay)
        ]

    def arrive(copies, g):
        for j in range(g * size, (g + 1) * size):
            if j:
                copies[j].wait_recv()

    def rows_of(buf, g):
        return buf[pl.ds(group[g] * size, size)].reshape(part, wide)

    def total(buf, g):
        whole = buf[0, group[g]].astype(F32)
        for i in range(1, n_lay):
            whole += buf[i, group[g]].astype(F32)
        return whole

    load_acts.wait()
    acts_copies = to_lat(acts_all, acts_s, acts_r)
    load_enc.wait()
    pre_copies, rec_copies = {}, {}

    def encode(g):
        arrive(acts_copies, g)
        pre = jnp.dot(rows_of(acts_all, g), wenc[...], preferred_element_type=F32)
        pre_buf[l, group[g]] = pre.astype(BF16)
        pre_copies[g] = to_lay(pre_buf, g, pre_s, pre_r)

    def decode(g):
        for copy in pre_copies[g]:
            copy.wait_recv()
        x = 4.0 * (total(pre_buf, g) + benc_ref[...].reshape(1, lat_dev))
        e = jnp.exp(-jnp.abs(x))
        code = (0.25 * (jnp.maximum(x, 0.0) + jnp.log1p(e))).astype(BF16)
        rec = jnp.dot(code, wdec[...], preferred_element_type=F32).astype(BF16)
        rec_mine[pl.ds(group[g] * size, size)] = rec.reshape(size, row_dev, wide)
        for j in range(g * size, (g + 1) * size):
            if j:
                rec_copies[j] = send(
                    rec_mine.at[dest(j)], rec_buf.at[z], rec_s.at[j], rec_r.at[j],
                    {"lat": dest(j)},
                )
        code_all[group[g]] = code
        slope[group[g]] = jnp.where(x >= 0.0, 1.0, e) / (1.0 + e)

    for g in range(groups):
        encode(g)
        if g == 0:
            load_dec.wait()
    for g in [*range(1, groups), 0]:
        decode(g)
    wdec_t[...] = wdec[...].astype(F32).T.astype(BF16)
    acts_t[...] = acts_all[...].reshape(rows, wide).astype(F32).T.astype(BF16)
    code_t = code_all[...].reshape(rows, lat_dev).astype(F32).T.astype(BF16)
    err = bdec_ref[...] - acts_all[z].astype(F32) + rec_mine[z].astype(F32)
    for j in range(1, n_lat):
        rec_copies[j].wait_recv()
        err += rec_buf[source(j)].astype(F32)
    err_all[z] = err.astype(BF16)
    err_copies = to_lat(err_all, err_s, err_r)
    back_copies = {}
    for g in range(groups):
        arrive(err_copies, g)
        back = jnp.dot(rows_of(err_all, g), wdec_t[...], preferred_element_type=F32)
        back_buf[l, group[g]] = back.astype(BF16)
        back_copies[g] = to_lay(back_buf, g, back_s, back_r)
    errs = err_all[...].reshape(rows, wide)
    dec_out[...] = jnp.dot(code_t, errs, preferred_element_type=F32).astype(BF16)
    for g in range(groups):
        for copy in back_copies[g]:
            copy.wait_recv()
        lat_out[group[g]] = (total(back_buf, g) * slope[group[g]]).astype(BF16)
    for copy in started:
        copy.wait_send()


def same(v, c):
    return lax.div(1, 1 + (v - c) * (v - c))


OWNER = [2, 2, 1, 0]
FIRST = [[0, 1, 2, 3], [1, 2, 3, 0], [2, 3, 1, 0], [3, 2, 1, 0]]
SECOND = [[3, 1, 2, 0], [2, 3, 1, 0], [0, 1, 2, 3], [1, 0, 2, 3]]
OWNED = [[3], [2], [1, 0], []]
TARGETS = [[3, 2, 1], [3, 2, 0], [0, 1, 3], [0, 1, 2]]
SPREAD = [[0, 1, 2, 3], [0, 3, 2, 1], [0, 3, 2], []]
LATER = [[], [], [(1, 1), (0, 1)], []]


def line_step(
    n_lat, n_lay, acts_hbm, wenc_hbm, wdec_hbm, benc_hbm, bdec_hbm,
    lat_out, acts_t, dec_out,
    acts_all, wenc, wdec, wdec_t, benc, bdec, pre_buf, back_buf, rec_mine, rec_buf, err_mine, err_all,
    code_all, slope,
    load, acts_s, acts_r, pre_s, pre_r, rec_s, rec_r, err_s, err_r, back_s, back_r,
):
    z, l = lax.axis_index("lat"), lax.axis_index("lay")
    row_dev, wide = acts_all.shape[1:]
    rows, lat_dev = n_lat * row_dev, wenc.shape[1]

    def pick(v, values):
        return sum(value * same(v, i) for i, value in enumerate(values))

    targets = [pick(z, [TARGETS[i][k] for i in range(n_lat)]) for k in range(n_lat - 1)]
    first = [pick(z, [FIRST[i][k] for i in range(n_lat)]) for k in range(n_lat)]
    second = [pick(z, [SECOND[i][k] for i in range(n_lat)]) for k in range(n_lat)]

    def lay_peer(k):
        return {"lay": flip(l, k)}

    odd = lax.rem(l, 2)
    barrier = pltpu.get_barrier_semaphore()
    for k in range(n_lat - 1):
        pl.semaphore_signal(barrier, inc=1, device_id={"lat": targets[k]}, device_id_type=MESH)
    for k in reversed(range(1, n_lay)):
        pl.semaphore_signal(barrier, inc=1, device_id=lay_peer(k), device_id_type=MESH)

    load_acts = pltpu.make_async_copy(acts_hbm, acts_all.at[z], load.at[0])
    load_enc = pltpu.make_async_copy(wenc_hbm, wenc, load.at[1])
    load_dec = pltpu.make_async_copy(wdec_hbm, wdec, load.at[2])
    load_benc = pltpu.make_async_copy(benc_hbm, benc, load.at[3])
    load_bdec = pltpu.make_async_copy(bdec_hbm, bdec, load.at[4])
    load_acts.start()
    load_enc.start()
    load_dec.start()
    load_benc.start()
    load_bdec.start()

    pl.semaphore_wait(barrier, n_lat + n_lay - 2)

    def send(src, dst, send_sem, recv_sem, peer):
        pltpu.make_async_remote_copy(
            src_ref=src, dst_ref=dst, send_sem=send_sem, recv_sem=recv_sem,
            device_id=peer, device_id_type=MESH,
        ).start()

    def wait(view, sem):
        pltpu.make_async_copy(view, view, sem).wait()

    def to_lay(buf, k, sent, received):
        for j in (2, 3):
            slot = j + odd * (5 - 2 * j)
            peer = flip(l, j) + odd * (flip(l, 5 - j) - flip(l, j))
            send(buf.at[k, 0], buf.at[k, slot], sent, received.at[k], {"lay": peer})
        send(buf.at[k, 0], buf.at[k, 1], sent, received.at[k], lay_peer(1))

    def total(buf, k, received):
        wait(buf.at[k, pl.ds(1, n_lay - 1)], received.at[k])
        whole = buf[k, l].astype(F32)
        for i in range(1, n_lay):
            whole += buf[k, flip(l, i)].astype(F32)
        return whole

    load_acts.wait()
    for k in range(n_lat - 1):
        send(acts_all.at[z], acts_all.at[z], acts_s, acts_r.at[z], {"lat": targets[k]})
    load_enc.wait()

    def encode(k):
        if k:
            wait(acts_all.at[first[k]], acts_r.at[first[k]])
        pre = jnp.dot(acts_all[first[k]], wenc[...], preferred_element_type=F32)
        pre_buf[k, 0] = pre.astype(BF16)
        to_lay(pre_buf, k, pre_s, pre_r)

    def decode(k):
        b = first[k]
        x = 4.0 * (total(pre_buf, k, pre_r) + benc[...].reshape(1, lat_dev))
        e = jnp.exp(-jnp.abs(x))
        code = (0.25 * (jnp.maximum(x, 0.0) + jnp.log1p(e))).astype(BF16)
        rec = jnp.dot(code, wdec[...], preferred_element_type=F32)
        owner = pick(b, OWNER)
        base = bdec[...] - acts_all[b].astype(F32)
        rec_mine[b] = (rec + jnp.where(owner == z, base, 0.0)).astype(BF16)

        @pl.when((odd == 0) | (owner != z))
        def _():
            peer = {"lat": owner, "lay": l + 1 - odd}
            send(rec_mine.at[b], rec_buf.at[odd, b, z], rec_s, rec_r.at[odd, b], peer)

        code_all[b] = code
        slope[b] = jnp.where(x >= 0.0, 1.0, e) / (1.0 + e)

    encode(0)
    load_dec.wait()
    wdec_t[...] = wdec[...].astype(F32).T.astype(BF16)
    for k in range(1, n_lat):
        encode(k)
    acts_t[...] = acts_all[...].reshape(rows, wide).astype(F32).T.astype(BF16)
    load_benc.wait()
    load_bdec.wait()
    for k in range(n_lat):
        decode(k)

    for i, owned in enumerate(OWNED):
        if owned:

            @pl.when((z == i) & (odd == 1))
            def _():
                for b in owned:
                    wait(rec_buf.at[0, b], rec_r.at[0, b])
                    err = rec_buf[0, b, 0].astype(F32)
                    for j in range(1, n_lat):
                        err += rec_buf[0, b, j].astype(F32)
                    err_mine[b] = err.astype(BF16)
                    for j in SPREAD[i]:
                        peer = {"lat": j, "lay": flip(l, 1)}
                        send(err_mine.at[b], err_all.at[b], err_s.at[0], err_r.at[b], peer)
                    wait(rec_buf.at[1, b, pl.ds(0, n_lat - 1)], rec_r.at[1, b])
                    err = rec_mine[b].astype(F32)
                    for j in range(n_lat):
                        if j != i:
                            err += rec_buf[1, b, j].astype(F32)
                    err_all[b] = err.astype(BF16)
                    for j in SPREAD[i]:
                        if j != i:
                            peer = {"lat": j}
                            send(err_all.at[b], err_all.at[b], err_s.at[1], err_r.at[b], peer)
                for b, j in LATER[i]:
                    peer = {"lat": j, "lay": flip(l, 1)}
                    send(err_mine.at[b], err_all.at[b], err_s.at[0], err_r.at[b], peer)
                    send(err_all.at[b], err_all.at[b], err_s.at[1], err_r.at[b], {"lat": j})

    code_t = code_all[...].reshape(rows, lat_dev).astype(F32).T.astype(BF16)
    for k in range(n_lat):
        b = second[k]

        @pl.when((odd == 0) | (pick(b, OWNER) != z))
        def _():
            wait(err_all.at[b], err_r.at[b])

        back = jnp.dot(err_all[b], wdec_t[...], preferred_element_type=F32)
        back_buf[k, 0] = back.astype(BF16)
        to_lay(back_buf, k, back_s, back_r)
    errs = err_all[...].reshape(rows, wide)
    dec_out[...] = jnp.dot(code_t, errs, preferred_element_type=F32).astype(BF16)
    for k in range(n_lat):
        b = second[k]
        lat_out[b] = (total(back_buf, k, back_r) * slope[b]).astype(BF16)

    wait(acts_all.at[pl.ds(0, n_lat - 1)], acts_s)
    wait(pre_buf.at[:, pl.ds(1, n_lay - 1)], pre_s)
    wait(back_buf.at[:, pl.ds(1, n_lay - 1)], back_s)
    @pl.when(odd == 0)
    def _():
        wait(rec_mine, rec_s)

    for i, owned in enumerate(OWNED):

        @pl.when((z == i) & (odd == 1))
        def _():
            wait(rec_mine.at[pl.ds(0, n_lat - len(owned))], rec_s)
            if owned:
                wait(rec_buf.at[0, pl.ds(0, len(owned))], err_s.at[0])
                wait(rec_buf.at[0, pl.ds(0, len(owned)), pl.ds(0, n_lat - 1)], err_s.at[1])


def finish(chunks, lat, acts_t, dec, lat_hbm, enc_hbm, dec_hbm, enc, sems):
    rows, lat_dev = lat.shape[0] * lat.shape[1], lat.shape[2]
    copies = [
        pltpu.make_async_copy(dec, dec_hbm, sems.at[0]),
        pltpu.make_async_copy(lat, lat_hbm, sems.at[1]),
    ]
    for copy in copies:
        copy.start()
    grad = lat[...].reshape(rows, lat_dev)
    tall = enc.shape[0] // chunks
    for c in range(chunks):
        cut = pl.ds(c * tall, tall)
        enc[cut] = jnp.dot(acts_t[cut], grad, preferred_element_type=F32).astype(BF16)
        copy = pltpu.make_async_copy(enc.at[cut], enc_hbm.at[cut], sems.at[2 + c])
        copy.start()
        copies.append(copy)
    for copy in copies:
        copy.wait()


def solution(mesh):
    n_lat, n_lay = mesh.shape["lat"], mesh.shape["lay"]

    def on_device(acts, w_enc, w_dec, b_enc, b_dec):
        row_dev, lay_dev, width = acts.shape
        lat_dev = w_enc.shape[2]
        wide, rows = lay_dev * width, n_lat * row_dev
        hbm = pl.BlockSpec(memory_space=pltpu.HBM)
        vmem = pl.BlockSpec(memory_space=pltpu.VMEM)
        dma = pltpu.SemaphoreType.DMA
        line = n_lat == len(OWNER) and n_lay == 4
        groups = 4 if n_lat & (n_lat - 1) == 0 and n_lat % 4 == 0 else 1
        if line:
            groups = n_lat
        part = rows // groups
        chunks = 5 if wide % 80 == 0 else 1
        out_shape = [
            pltpu.VMEM((groups, part, lat_dev), BF16),
            pltpu.VMEM((wide, rows), BF16),
            pltpu.VMEM((lat_dev, wide), BF16),
        ]
        rows_buf = pltpu.VMEM((n_lat, row_dev, wide), BF16)
        if line:
            kernel = functools.partial(line_step, n_lat, n_lay)
            in_specs = [hbm] * 5
            lay_buf = pltpu.VMEM((groups, n_lay, part, lat_dev), BF16)
            scratch = [
                rows_buf,
                pltpu.VMEM((wide, lat_dev), BF16),
                pltpu.VMEM((lat_dev, wide), BF16),
                pltpu.VMEM((wide, lat_dev), BF16),
                pltpu.VMEM((lat_dev,), F32),
                pltpu.VMEM((1, wide), F32),
                lay_buf,
                lay_buf,
                rows_buf,
                pltpu.VMEM((2, n_lat, n_lat, row_dev, wide), BF16),
                rows_buf,
                rows_buf,
                pltpu.VMEM((groups, part, lat_dev), BF16),
                pltpu.VMEM((groups, part, lat_dev), F32),
                dma((5,)),
                dma, dma((n_lat,)),
                dma, dma((groups,)),
                dma, dma((2, n_lat)),
                dma((2,)), dma((n_lat,)),
                dma, dma((groups,)),
            ]
        else:
            kernel = functools.partial(step, n_lat, n_lay, groups)
            in_specs = [hbm, hbm, hbm, vmem, vmem]
            scratch = [
                rows_buf,
                pltpu.VMEM((wide, lat_dev), BF16),
                pltpu.VMEM((lat_dev, wide), BF16),
                pltpu.VMEM((wide, lat_dev), BF16),
                pltpu.VMEM((n_lay, groups, part, lat_dev), BF16),
                pltpu.VMEM((n_lay, groups, part, lat_dev), BF16),
                rows_buf,
                rows_buf,
                rows_buf,
                pltpu.VMEM((groups, part, lat_dev), BF16),
                pltpu.VMEM((groups, part, lat_dev), F32),
                dma((3,)),
                dma((n_lat,)), dma((n_lat,)),
                dma((groups, n_lay)), dma((groups, n_lay)),
                dma((n_lat,)), dma((n_lat,)),
                dma((n_lat,)), dma((n_lat,)),
                dma((groups, n_lay)), dma((groups, n_lay)),
            ]
        lat_part, acts_t, dec_part = pl.pallas_call(
            kernel,
            out_shape=out_shape,
            in_specs=in_specs,
            out_specs=[vmem, vmem, vmem],
            scratch_shapes=scratch,
            compiler_params=pltpu.CompilerParams(collective_id=0, has_side_effects=True),
            cost_estimate=pl.CostEstimate(
                flops=8 * rows * wide * lat_dev,
                bytes_accessed=4 * wide * lat_dev,
                transcendentals=0,
            ),
        )(
            acts.reshape(row_dev, wide),
            w_enc.reshape(wide, lat_dev),
            w_dec.reshape(lat_dev, wide),
            b_enc,
            b_dec.reshape(1, wide),
        )
        lat_grad, enc_grad, dec_grad = pl.pallas_call(
            functools.partial(finish, chunks),
            out_shape=[
                jax.ShapeDtypeStruct((groups, part, lat_dev), BF16),
                jax.ShapeDtypeStruct((wide, lat_dev), BF16),
                jax.ShapeDtypeStruct((lat_dev, wide), BF16),
            ],
            in_specs=[vmem, vmem, vmem],
            out_specs=[hbm, hbm, hbm],
            scratch_shapes=[pltpu.VMEM((wide, lat_dev), BF16), dma((2 + chunks,))],
            compiler_params=pltpu.CompilerParams(vmem_limit_bytes=8 * wide * lat_dev),
            cost_estimate=pl.CostEstimate(
                flops=2 * rows * wide * lat_dev,
                bytes_accessed=4 * wide * lat_dev,
                transcendentals=0,
            ),
        )(lat_part, acts_t, dec_part)
        return (
            lat_grad.reshape(rows, lat_dev),
            enc_grad.reshape(lay_dev, width, lat_dev),
            dec_grad.reshape(lat_dev, lay_dev, width),
        )

    in_specs = (
        P(("grp", "lat"), "lay", None),
        P("lay", None, "lat"),
        P("lat", "lay", None),
        P("lat"),
        P("lay", None),
    )
    out_specs = (P("grp", "lat"), P(("grp", "lay"), None, "lat"), P("lat", ("grp", "lay"), None))
    return jax.shard_map(
        on_device, mesh=mesh, in_specs=in_specs, out_specs=out_specs, check_vma=False
    )
```
